32 devices in a mesh: groups: 2 (over y), dp: 4 (over x, core), tensor: 4 (over z).
Axes of the slice: x: 2, y: 2, z: 4, core: 2. Of those that a mesh axis runs over, the one named last changes fastest.
Arguments:
- tokens: bfloat16 [1024, 8192], P(('groups', 'dp'), 'tensor'), parts along dimension 0, may hold values from -6 to 6
- gate_up_weight: bfloat16 [8192, 2048], P('dp', 'tensor'), may hold values from -0.0625 to 0.0625
- down_weight: bfloat16 [1024, 8192], P('tensor', 'dp'), may hold values from -0.1875 to 0.1875
Outputs:
- mixed_out: bfloat16 [1024, 8192], P(('groups', 'dp'), 'tensor'), parts along dimension 0
The draws below stay inside these ranges and needn't reach their ends.
There are 2 independent parts, one for each index of `groups`. The reference program is written for one: setup_inputs(seed, part) draws one part's arguments, and reference() takes and returns one part's arrays. A program takes and returns all parts, laid end to end along the dimension named above; an argument that names none is the same for every part. Nothing has to cross between parts.
All inputs are finite; a program needn't handle non-finite values.
Results may differ from the reference program's by a relative error of at most 0.0049.
Values may be sent and summed in bfloat16 or wider, within the bound.
A program may use at most 64 MiB of HBM per device.

```python
import jax
import jax.numpy as jnp

D = 8192
FF = 1024
TOKENS = 512


def block_levels(rng, dims, shards, low, top_value):
    def one(axis_at, blocks):
        steps = jax.random.uniform(jax.random.fold_in(jax.random.fold_in(rng, 6), axis_at), (blocks,), jnp.float32, low / len(shards), top_value / len(shards))
        return jnp.repeat(jnp.exp(steps), dims[axis_at] // blocks).reshape((-1,) + (1,) * (len(dims) - axis_at - 1))

    level = one(*shards[0])
    for cut in shards[1:]:
        level = level * one(*cut)
    return level


def bell_draw(stream_key, extent, deviation, bound, shards=(), dtype=jnp.bfloat16):
    entries = deviation * jax.random.normal(stream_key, extent, jnp.float32)
    if shards:
        entries = entries * block_levels(stream_key, extent, shards, -0.22, 0.18)
    return jnp.clip(entries, -bound, bound).astype(dtype)


def setup_inputs(seed: int = 0, part: int = 0) -> dict:
    keys = jax.random.split(jax.random.key(seed), 4)
    part_splits = jax.random.split(jax.random.fold_in(keys[3], part), 4)
    tokens = bell_draw(part_splits[0], (TOKENS, D), 1.0, 6.0, ((0, 4), (1, 4)))
    gate_up_weight = bell_draw(keys[1], (D, 2 * FF), D ** -0.5, 0.0625, ((0, 4), (1, 4)))
    down_weight = bell_draw(keys[2], (FF, D), FF ** -0.5, 0.1875, ((0, 4), (1, 4)))
    return {"tokens": tokens, "gate_up_weight": gate_up_weight, "down_weight": down_weight}


def reference(tokens, gate_up_weight, down_weight):
    combined = jnp.dot(tokens, gate_up_weight, preferred_element_type=jnp.float32)
    gate_part = combined[:, 0::2]
    up_part = combined[:, 1::2]
    hidden = (jax.nn.silu(gate_part) * up_part).astype(jnp.bfloat16)
    return jnp.dot(hidden, down_weight, preferred_element_type=jnp.float32).astype(jnp.bfloat16)
```

```python
import functools

import jax
import jax.numpy as jnp
from jax import lax
from jax.experimental import pallas as pl
from jax.experimental.pallas import tpu as pltpu
from jax.sharding import PartitionSpec as P

MESH = pl.DeviceIdType.MESH
EARLY = 0
XE = 1
HELD = 0
BEGIN, GX, GY, DX, DZ, CX, FAR = 7.0, 8.5, 12.1, 2.8, 16.0, 31.0, 20.0
TOK0, TOK, DTOK = 8.0, 14.0, 5.7


def loop(first, last, body):
    if last - first <= 8:
        for step in range(first, last):
            body(step)
    else:
        lax.fori_loop(first, last, lambda step, _: (body(step), 0)[1], 0)


def when(condition, body):
    pl.when(condition)(body)


def kernel(sizes, tok_in, gu_in, dn_in, out, tok, gu, stage, down, hid, comb, acc,
           s_loc, s_tok, s_own, s_gx, s_gy, s_glx, s_gly, s_da, s_db, s_cx, s_cy, s_cl, s_hid, s_cf, s_far, s_gf):
    G, N, T, L, H, NC, TC = sizes
    g, d, t = lax.axis_index("groups"), lax.axis_index("dp"), lax.axis_index("tensor")
    hi, lo = d // L, lax.rem(d, L)
    rows, feats = tok_in.shape
    depth, width = gu_in.shape
    units, _ = dn_in.shape
    cols = out.shape[1]
    sub = dn_in.shape[1] // cols
    piece = depth // G
    chunk = piece // NC
    quarter = units // N
    part = quarter // G
    trow = rows // TC

    def at(axis, index):
        return {axis: index}

    def remote(src, dst, sem, index, device):
        return pltpu.make_async_remote_copy(
            src_ref=src, dst_ref=dst, send_sem=sem.at[(0,) + index], recv_sem=sem.at[(1,) + index],
            device_id=device, device_id_type=MESH,
        )

    def dp_of(h, l):
        return lax.rem(h + 2 * H, H) * L + l

    other = dp_of(hi, lax.rem(lo + 1, L))

    barrier = pltpu.get_barrier_semaphore()
    peers = 0
    for k in range(1, N):
        pl.semaphore_signal(barrier, inc=1, device_id=at("dp", lax.rem(d + k, N)), device_id_type=MESH)
        peers += 1
    for k in range(1, G):
        pl.semaphore_signal(barrier, inc=1, device_id=at("groups", lax.rem(g + k, G)), device_id_type=MESH)
        peers += 1

    def greet(k):
        pl.semaphore_signal(barrier, inc=1, device_id=at("tensor", lax.rem(t + k, T)), device_id_type=MESH)

    line = T <= 8
    below, above = t > 0, t + 1 < T

    def beside(ok, step, sem):
        when(ok, lambda: pl.semaphore_signal(sem, inc=1, device_id=at("tensor", t + step), device_id_type=MESH))

    if line:
        beside(above, 1, barrier)
        beside(below, -1, barrier)
        peers += jnp.where(below, 1, 0) + jnp.where(above, 1, 0)
    else:
        loop(1, T, greet)
        peers += T - 1

    own_tok = pltpu.make_async_copy(tok_in, tok.at[:, pl.ds(pl.multiple_of(t * feats, 128), feats)], s_loc.at[0])
    own_gu = pltpu.make_async_copy(gu_in, gu.at[d], s_loc.at[1])

    def share(dd, gg):
        return pl.ds(pl.multiple_of(dd * quarter + gg * part, 16), part)

    own_stage = pltpu.make_async_copy(dn_in.at[share(d, g)], stage.at[d], s_loc.at[2])
    own_tok.start()
    own_gu.start()
    own_stage.start()
    pl.semaphore_wait(barrier, peers)

    def tok_block(b, c):
        return tok.at[pl.ds(c * trow, trow), pl.ds(pl.multiple_of(b * feats, 128), feats)]

    def tok_send(way, s, c, first):
        b = t - (s - 1) if way == 0 else t + (s - 1)
        dst = tok_block(b, c)
        src = tok_in.at[pl.ds(c * trow, trow)] if first else dst
        return remote(src, dst, s_tok, (way, s - 1, c), at("tensor", t + 1 if way == 0 else t - 1))

    def tok_can_send(way, s):
        if way == 0:
            return jnp.logical_and(t + 1 < T, t - (s - 1) >= 0)
        return jnp.logical_and(t - 1 >= 0, t + (s - 1) < T)

    def tok_recv(way, s, c):
        b = t - s if way == 0 else t + s
        dst = tok_block(b, c)
        return remote(dst, dst, s_tok, (way, s - 1, c), at("tensor", t))

    def tok_has(way, s):
        return t - s >= 0 if way == 0 else t + s < T

    def tok_step(s, c):
        for way in range(2):
            def arrive(way=way):
                tok_recv(way, s, c).wait_recv()

                def forward():
                    tok_send(way, s + 1, c, False).start()

                when(tok_can_send(way, s + 1), forward)

            when(tok_has(way, s), arrive)

    def gu_at(dd, gg, c):
        return gu.at[dd, pl.ds(pl.multiple_of(gg * piece + c * chunk, 16), chunk)]

    def gx(k, c, to):
        if to:
            src = gu_in.at[pl.ds(pl.multiple_of(g * piece + c * chunk, 16), chunk)]
            return remote(src, gu_at(d, g, c), s_gx, (k - 1, c), at("dp", dp_of(hi + k, lo)))
        ref = gu_at(dp_of(hi - k, lo), g, c)
        return remote(ref, ref, s_gx, (k - 1, c), at("dp", d))

    def gf(k, q, c, to):
        far = lax.rem(g - q + G, G)
        if to:
            src = gu_in.at[pl.ds(pl.multiple_of(far * piece + c * chunk, 16), chunk)]
            return remote(src, gu_at(d, far, c), s_gf, (k - 1, q - 1, c), at("dp", dp_of(hi + k, lo)))
        ref = gu_at(dp_of(hi - k, lo), far, c)
        return remote(ref, ref, s_gf, (k - 1, q - 1, c), at("dp", d))

    def gy(k, q, c, to):
        ref = gu_at(dp_of(hi - k, lo), g if to else lax.rem(g - q + G, G), c)
        return remote(ref, ref, s_gy, (k - 1, q - 1, c), at("groups", lax.rem(g + q, G)))

    def glx(k, c, to):
        ref = gu_at(dp_of(hi - k, lo if to else lax.rem(lo + 1, L)), g, c)
        return remote(ref, ref, s_glx, (k - 1, c), at("dp", other))

    def gly(k, q, c, to):
        ref = gu_at(dp_of(hi - k, lo if to else lax.rem(lo + 1, L)), lax.rem(g - q + G, G), c)
        return remote(ref, ref, s_gly, (k - 1, q - 1, c), at("dp", other))

    def own_share(to):
        return remote(gu_in, gu.at[d] if to else gu.at[other], s_own, (0,), at("dp", other))

    def da(k, to):
        if to:
            dd = lax.rem(d + k, N)
            return remote(dn_in.at[share(dd, g)], stage.at[d], s_da, (k - 1,), at("dp", dd))
        ref = stage.at[lax.rem(d - k + N, N)]
        return remote(ref, ref, s_da, (k - 1,), at("dp", d))

    def staged(tt):
        return stage.at[tt // sub, :, pl.ds(pl.multiple_of(lax.rem(tt, sub) * cols, 128), cols)]

    def db(k, to):
        tt = lax.rem(t + k, T)
        if to:
            return remote(staged(tt), down.at[t, share(d, g)], s_db, (k - 1,), at("tensor", tt))
        ref = down.at[lax.rem(t - k + T, T), share(d, g)]
        return remote(ref, ref, s_db, (k - 1,), at("tensor", t))

    def cx(k, m, to):
        tt = lax.rem(t - k + T, T)
        ref = down.at[tt, share(d if to else dp_of(hi - m, lo), g)]
        return remote(ref, ref, s_cx, (m - 1, k), at("dp", dp_of(hi + m, lo)))

    def cy(k, m, q, to):
        tt = lax.rem(t - k + T, T)
        ref = down.at[tt, share(dp_of(hi - m, lo), g if to else lax.rem(g - q + G, G))]
        return remote(ref, ref, s_cy, (q - 1, m, k), at("groups", lax.rem(g + q, G)))

    def cf(m, q, to):
        far = lax.rem(g - q + G, G)
        ref = down.at[t, share(d if to else dp_of(hi - m, lo), far)]
        return remote(ref, ref, s_cf, (q - 1, m - 1), at("dp", dp_of(hi + m, lo)))

    def far_half():
        for q in range(1, G):
            cy(0, 0, q, False).wait_recv()
            for m in range(1, H):
                cf(m, q, True).start()

    def cl(k, m, to):
        tt = lax.rem(t - k + T, T)
        dd = dp_of(hi - m, lo if to else lax.rem(lo + 1, L))
        ref = down.at[tt, pl.ds(pl.multiple_of(dd * quarter, 16), quarter)]
        return remote(ref, ref, s_cl, (m, k), at("dp", other))

    def tok_first(c):
        for way in range(2):
            when(tok_can_send(way, 1), lambda way=way: tok_send(way, 1, c, True).start())

    for c in range(HELD, TC):
        tok_first(c)
    for c in range(NC):
        if c == EARLY:
            for k in range(1, N):
                da(k, True).start()
        for k in range(1, H):
            gx(k, c, True).start()
    for c in range(NC - XE, NC):
        for k in range(1, H):
            for q in range(1, G):
                gf(k, q, c, True).start()
    if L > 1:
        own_share(True).start()

    def gu_x(c):
        for k in range(1, H):
            gx(k, c, False).wait_recv()
            for q in range(1, G) if c < NC - XE else ():
                gy(k, q, c, True).start()
            if L > 1:
                glx(k, c, True).start()

    def gu_y(c):
        for k in range(1, H):
            for q in range(1, G):
                (gy if c < NC - XE else gf)(k, q, c, False).wait_recv()
                if L > 1:
                    gly(k, q, c, True).start()

    def meet():
        when(below, lambda: pl.semaphore_wait(s_far.at[0], 1))
        beside(above, 1, s_far.at[0])
        when(above, lambda: pl.semaphore_wait(s_far.at[1], 1))
        beside(below, -1, s_far.at[1])

    if line:
        meet()

    def dispatch():
        own_stage.wait()
        for k in range(1, N):
            da(k, False).wait_recv()
        loop(1, T, lambda k: db(k, True).start())
        mine = pltpu.make_async_copy(staged(t), down.at[t, share(d, g)], s_loc.at[2])
        mine.start()
        mine.wait()

    def down_z(k, mine):
        if not mine:
            db(k, False).wait_recv()
        for m in range(1, H):
            cx(k, m, True).start()
        for q in range(1, G):
            cy(k, 0, q, True).start()

    def down_x(k, mine=False):
        for m in range(1, H):
            cx(k, m, False).wait_recv()
            for q in () if mine else range(1, G):
                cy(k, m, q, True).start()

    def down_y(k, mine=False):
        for m in range(H):
            for q in range(1, G):
                if not mine:
                    cy(k, m, q, False).wait_recv()
                elif m:
                    cf(m, q, False).wait_recv()
            if L > 1:
                cl(k, m, True).start()

    def gu_all():
        own_gu.wait()
        if L > 1:
            own_share(False).wait_recv()
            for k in range(1, H):
                for c in range(NC):
                    glx(k, c, False).wait_recv()
                    for q in range(1, G):
                        gly(k, q, c, False).wait_recv()

    def product(b):
        at_b = pl.ds(pl.multiple_of(b * feats, 128), feats)
        return jnp.dot(tok[:, at_b], gu[b * feats // depth, pl.ds(pl.multiple_of(lax.rem(b * feats, depth), 128), feats)],
                       preferred_element_type=jnp.float32)

    def near(s):
        def below():
            comb[...] += product(t - s)

        def above():
            comb[...] += product(t + s)

        when(t - s >= 0, below)
        when(t + s < T, above)

    def first_products():
        gu_all()
        comb[...] = product(t)
        for s in range(1, T - 1):
            near(s)

    def begin():
        dispatch()
        for c in range(HELD):
            tok_first(c)
        down_z(0, True)

    if T <= 8:
        own_tok.wait()
        events = [(BEGIN, begin)]
        events += [(GX + DX * c, functools.partial(gu_x, c)) for c in range(NC)]
        events += [(GY + DX * c, functools.partial(gu_y, c)) for c in range(NC)]
        events += [(GY + DX * NC + 2.0, first_products)]
        events += [(DZ + 2.0 * k, functools.partial(down_z, k, False)) for k in range(1, T)]
        events += [(TOK0 if (s, c) == (1, 0) else TOK + DTOK * ((s - 1) * TC + c), functools.partial(tok_step, s, c))
                   for s in range(1, T) for c in range(TC)]
        events += [(CX + DX * k, functools.partial(down_x, k, k == 0)) for k in range(T)]
        events += [(FAR, far_half)]
        for _, event in sorted(events, key=lambda e: e[0]):
            event()
        near(T - 1)
    else:
        own_tok.wait()
        for c in range(NC):
            gu_x(c)
        begin()
        for c in range(NC):
            gu_y(c)

        def whole_step(s):
            for c in range(TC):
                tok_step(s, c)

        loop(1, T, whole_step)
        loop(1, T, lambda k: down_z(k, False))
        far_half()
        down_x(0, True)
        loop(1, T, down_x)
        gu_all()
        comb[...] = product(t)
        loop(1, T, near)

    total = comb[...]
    up = pltpu.roll(total, width - 1, 1)
    wide = total / (1.0 + jnp.exp(-total)) * up
    even = lax.rem(lax.broadcasted_iota(jnp.int32, wide.shape, 1), 2) == 0
    wide = jnp.where(even, wide, 0.0).astype(jnp.bfloat16)
    pick = (lax.broadcasted_iota(jnp.int32, (width, units), 0)
            == 2 * lax.broadcasted_iota(jnp.int32, (width, units), 1))
    pick = jnp.where(pick, 1.0, 0.0).astype(jnp.bfloat16)
    hid[t] = jnp.dot(wide, pick, preferred_element_type=jnp.float32).astype(jnp.bfloat16)

    def hs(k, to):
        ref = hid.at[t if to else lax.rem(t - k + T, T)]
        return remote(ref, ref, s_hid, (k - 1,), at("tensor", lax.rem(t + k, T)))

    loop(1, T, lambda k: hs(k, True).start())
    down_y(0, True)
    loop(1, T, down_y)
    if L > 1:
        def shared(k):
            for m in range(H):
                cl(k, m, False).wait_recv()
        loop(0, T, shared)

    acc[...] = jnp.dot(hid[t], down[t], preferred_element_type=jnp.float32)

    def mix(k):
        hs(k, False).wait_recv()
        tt = lax.rem(t - k + T, T)
        acc[...] += jnp.dot(hid[tt], down[tt], preferred_element_type=jnp.float32)

    loop(1, T, mix)
    out[...] = acc[...].astype(out.dtype)

    def tok_sent(s):
        for way in range(2):
            for c in range(TC):
                when(tok_can_send(way, s), lambda way=way, c=c: tok_send(way, s, c, False).wait_send())

    loop(1, T, tok_sent)
    for k in range(1, H):
        for c in range(NC):
            gx(k, c, True).wait_send()
            if L > 1:
                glx(k, c, True).wait_send()
            for q in range(1, G):
                (gy if c < NC - XE else gf)(k, q, c, True).wait_send()
                if L > 1:
                    gly(k, q, c, True).wait_send()
    if L > 1:
        own_share(True).wait_send()
    for k in range(1, N):
        da(k, True).wait_send()

    def sent(k):
        db(k, True).wait_send()
        hs(k, True).wait_send()

    loop(1, T, sent)

    def plane_sent(k, mine=False):
        for m in range(1, H):
            cx(k, m, True).wait_send()
        for m in range(H):
            for q in range(1, G):
                if mine and m:
                    cf(m, q, True).wait_send()
                else:
                    cy(k, m, q, True).wait_send()
            if L > 1:
                cl(k, m, True).wait_send()

    plane_sent(0, True)
    loop(1, T, plane_sent)


def per_device(mesh, tokens, gate_up_weight, down_weight):
    G, N, T = (mesh.shape[a] for a in ("groups", "dp", "tensor"))
    L = 2 if N % 2 == 0 else 1
    H = N // L
    NC, TC = 8, 2
    rows, feats = tokens.shape
    depth, width = gate_up_weight.shape
    units = down_weight.shape[0]
    cols = down_weight.shape[1] * N // T
    dma = pltpu.SemaphoreType.DMA
    one = max
    bf = jnp.bfloat16
    sem = lambda *shape: dma((2,) + tuple(one(1, n) for n in shape))
    return pl.pallas_call(
        functools.partial(kernel, (G, N, T, L, H, NC, TC)),
        out_shape=jax.ShapeDtypeStruct((rows, cols), bf),
        in_specs=[pl.BlockSpec(memory_space=pl.ANY)] * 3,
        out_specs=pl.BlockSpec(memory_space=pltpu.VMEM),
        scratch_shapes=[
            pltpu.VMEM((rows, feats * T), bf),
            pltpu.VMEM((N, depth, width), bf),
            pltpu.VMEM((N, units // N // G, down_weight.shape[1]), bf),
            pltpu.VMEM((T, units, cols), bf),
            pltpu.VMEM((T, rows, units), bf),
            pltpu.VMEM((rows, width), jnp.float32),
            pltpu.VMEM((rows, cols), jnp.float32),
            dma((3,)),
            sem(2, T - 1, TC),
            sem(1),
            sem(H - 1, NC),
            sem(H - 1, G - 1, NC),
            sem(H - 1, NC),
            sem(H - 1, G - 1, NC),
            sem(N - 1),
            sem(T - 1),
            sem(H - 1, T),
            sem(G - 1, H, T),
            sem(H, T),
            sem(T - 1),
            sem(G - 1, H - 1),
            pltpu.SemaphoreType.REGULAR((2,)),
            sem(H - 1, G - 1, NC),
        ],
        compiler_params=pltpu.CompilerParams(collective_id=0, has_side_effects=True,
                                             vmem_limit_bytes=60 * 1024 * 1024),
    )(tokens, gate_up_weight, down_weight)


def solution(mesh):
    in_specs = (P(("groups", "dp"), "tensor"), P("dp", "tensor"), P("tensor", "dp"))
    out_specs = P(("groups", "dp"), "tensor")
    return jax.shard_map(
        functools.partial(per_device, mesh), mesh=mesh, in_specs=in_specs, out_specs=out_specs, check_vma=False
    )
```

```python
import functools

import jax
import jax.numpy as jnp
from jax import lax
from jax.experimental import pallas as pl
from jax.experimental.pallas import tpu as pltpu
from jax.sharding import PartitionSpec as P

MESH = pl.DeviceIdType.MESH
EARLY = 0
XE = 1
HELD = 0
BEGIN, GX, GY, DX, DZ, CX, FAR = 7.0, 8.5, 12.1, 2.8, 18.0, 31.0, 20.0
DDZ, DCX, PROD = 2.0, 2.8, 36.5
TOK0, TOK, DTOK = 8.0, 14.0, 5.7


def loop(first, last, body):
    if last - first <= 8:
        for step in range(first, last):
            body(step)
    else:
        lax.fori_loop(first, last, lambda step, _: (body(step), 0)[1], 0)


def when(condition, body):
    pl.when(condition)(body)


def kernel(sizes, tok_in, gu_in, dn_in, out, tok, gu, stage, down, hid, comb, acc,
           s_loc, s_tok, s_own, s_gx, s_gy, s_glx, s_gly, s_da, s_db, s_cx, s_cy, s_cl, s_hid, s_cf, s_far, s_gf):
    G, N, T, L, H, NC, TC = sizes
    g, d, t = lax.axis_index("groups"), lax.axis_index("dp"), lax.axis_index("tensor")
    hi, lo = d // L, lax.rem(d, L)
    rows, feats = tok_in.shape
    depth, width = gu_in.shape
    units, _ = dn_in.shape
    cols = out.shape[1]
    sub = dn_in.shape[1] // cols
    piece = depth // G
    chunk = piece // NC
    quarter = units // N
    part = quarter // G
    trow = rows // TC

    def at(axis, index):
        return {axis: index}

    def remote(src, dst, sem, index, device):
        return pltpu.make_async_remote_copy(
            src_ref=src, dst_ref=dst, send_sem=sem.at[(0,) + index], recv_sem=sem.at[(1,) + index],
            device_id=device, device_id_type=MESH,
        )

    def dp_of(h, l):
        return lax.rem(h + 2 * H, H) * L + l

    other = dp_of(hi, lax.rem(lo + 1, L))

    barrier = pltpu.get_barrier_semaphore()
    peers = 0
    for k in range(1, N):
        pl.semaphore_signal(barrier, inc=1, device_id=at("dp", lax.rem(d + k, N)), device_id_type=MESH)
        peers += 1
    for k in range(1, G):
        pl.semaphore_signal(barrier, inc=1, device_id=at("groups", lax.rem(g + k, G)), device_id_type=MESH)
        peers += 1

    def greet(k):
        pl.semaphore_signal(barrier, inc=1, device_id=at("tensor", lax.rem(t + k, T)), device_id_type=MESH)

    line = T <= 8
    below, above = t > 0, t + 1 < T

    def beside(ok, step, sem):
        when(ok, lambda: pl.semaphore_signal(sem, inc=1, device_id=at("tensor", t + step), device_id_type=MESH))

    if line:
        beside(above, 1, barrier)
        beside(below, -1, barrier)
        peers += jnp.where(below, 1, 0) + jnp.where(above, 1, 0)
    else:
        loop(1, T, greet)
        peers += T - 1

    own_tok = pltpu.make_async_copy(tok_in, tok.at[:, pl.ds(pl.multiple_of(t * feats, 128), feats)], s_loc.at[0])
    own_gu = pltpu.make_async_copy(gu_in, gu.at[d], s_loc.at[1])

    def share(dd, gg):
        return pl.ds(pl.multiple_of(dd * quarter + gg * part, 16), part)

    own_stage = pltpu.make_async_copy(dn_in.at[share(d, g)], stage.at[d], s_loc.at[2])
    own_tok.start()
    own_gu.start()
    own_stage.start()
    pl.semaphore_wait(barrier, peers)

    def nearest(j, late):
        pick = 0
        for here in range(T):
            order = sorted((p for p in range(T) if p != here),
                           key=lambda p: (late and p in (0, T - 1), abs(p - here)))
            pick = jnp.where(t == here, order[j - 1], pick)
        return lax.rem(t - pick + T, T)

    def tok_block(b, c):
        return tok.at[pl.ds(c * trow, trow), pl.ds(pl.multiple_of(b * feats, 128), feats)]

    def tok_send(way, s, c, first):
        b = t - (s - 1) if way == 0 else t + (s - 1)
        dst = tok_block(b, c)
        src = tok_in.at[pl.ds(c * trow, trow)] if first else dst
        return remote(src, dst, s_tok, (way, s - 1, c), at("tensor", t + 1 if way == 0 else t - 1))

    def tok_can_send(way, s):
        if way == 0:
            return jnp.logical_and(t + 1 < T, t - (s - 1) >= 0)
        return jnp.logical_and(t - 1 >= 0, t + (s - 1) < T)

    def tok_recv(way, s, c):
        b = t - s if way == 0 else t + s
        dst = tok_block(b, c)
        return remote(dst, dst, s_tok, (way, s - 1, c), at("tensor", t))

    def tok_has(way, s):
        return t - s >= 0 if way == 0 else t + s < T

    def last_plane():
        return jnp.logical_or(t == 0, t == T - 1)

    def tok_step(s, c):
        for way in range(2):
            def arrive(way=way):
                tok_recv(way, s, c).wait_recv()

                def forward():
                    tok_send(way, s + 1, c, False).start()

                when(tok_can_send(way, s + 1), forward)

            met = tok_has(way, s)
            when(jnp.logical_and(met, jnp.logical_not(last_plane())) if line else met, arrive)

    def gu_at(dd, gg, c):
        return gu.at[dd, pl.ds(pl.multiple_of(gg * piece + c * chunk, 16), chunk)]

    def gx(k, c, to):
        if to:
            src = gu_in.at[pl.ds(pl.multiple_of(g * piece + c * chunk, 16), chunk)]
            return remote(src, gu_at(d, g, c), s_gx, (k - 1, c), at("dp", dp_of(hi + k, lo)))
        ref = gu_at(dp_of(hi - k, lo), g, c)
        return remote(ref, ref, s_gx, (k - 1, c), at("dp", d))

    def gf(k, q, c, to):
        far = lax.rem(g - q + G, G)
        if to:
            src = gu_in.at[pl.ds(pl.multiple_of(far * piece + c * chunk, 16), chunk)]
            return remote(src, gu_at(d, far, c), s_gf, (k - 1, q - 1, c), at("dp", dp_of(hi + k, lo)))
        ref = gu_at(dp_of(hi - k, lo), far, c)
        return remote(ref, ref, s_gf, (k - 1, q - 1, c), at("dp", d))

    def gy(k, q, c, to):
        ref = gu_at(dp_of(hi - k, lo), g if to else lax.rem(g - q + G, G), c)
        return remote(ref, ref, s_gy, (k - 1, q - 1, c), at("groups", lax.rem(g + q, G)))

    def glx(k, c, to):
        ref = gu_at(dp_of(hi - k, lo if to else lax.rem(lo + 1, L)), g, c)
        return remote(ref, ref, s_glx, (k - 1, c), at("dp", other))

    def gly(k, q, c, to):
        ref = gu_at(dp_of(hi - k, lo if to else lax.rem(lo + 1, L)), lax.rem(g - q + G, G), c)
        return remote(ref, ref, s_gly, (k - 1, q - 1, c), at("dp", other))

    def own_share(to):
        return remote(gu_in, gu.at[d] if to else gu.at[other], s_own, (0,), at("dp", other))

    def da(k, to):
        if to:
            dd = lax.rem(d + k, N)
            return remote(dn_in.at[share(dd, g)], stage.at[d], s_da, (k - 1,), at("dp", dd))
        ref = stage.at[lax.rem(d - k + N, N)]
        return remote(ref, ref, s_da, (k - 1,), at("dp", d))

    def staged(tt):
        return stage.at[tt // sub, :, pl.ds(pl.multiple_of(lax.rem(tt, sub) * cols, 128), cols)]

    def db(k, to):
        tt = lax.rem(t + k, T)
        if to:
            return remote(staged(tt), down.at[t, share(d, g)], s_db, (k - 1,), at("tensor", tt))
        ref = down.at[lax.rem(t - k + T, T), share(d, g)]
        return remote(ref, ref, s_db, (k - 1,), at("tensor", t))

    def cx(k, m, to):
        tt = lax.rem(t - k + T, T)
        ref = down.at[tt, share(d if to else dp_of(hi - m, lo), g)]
        return remote(ref, ref, s_cx, (m - 1, k), at("dp", dp_of(hi + m, lo)))

    def cy(k, m, q, to):
        tt = lax.rem(t - k + T, T)
        ref = down.at[tt, share(dp_of(hi - m, lo), g if to else lax.rem(g - q + G, G))]
        return remote(ref, ref, s_cy, (q - 1, m, k), at("groups", lax.rem(g + q, G)))

    def cf(m, q, to):
        far = lax.rem(g - q + G, G)
        ref = down.at[t, share(d if to else dp_of(hi - m, lo), far)]
        return remote(ref, ref, s_cf, (q - 1, m - 1), at("dp", dp_of(hi + m, lo)))

    def far_half():
        for q in range(1, G):
            cy(0, 0, q, False).wait_recv()
            for m in range(1, H):
                cf(m, q, True).start()

    def cl(k, m, to):
        tt = lax.rem(t - k + T, T)
        dd = dp_of(hi - m, lo if to else lax.rem(lo + 1, L))
        ref = down.at[tt, pl.ds(pl.multiple_of(dd * quarter, 16), quarter)]
        return remote(ref, ref, s_cl, (m, k), at("dp", other))

    def tok_first(c):
        for way in range(2):
            when(tok_can_send(way, 1), lambda way=way: tok_send(way, 1, c, True).start())

    for c in range(HELD, TC):
        tok_first(c)
    for c in range(NC):
        if c == EARLY:
            for k in range(1, N):
                da(k, True).start()
        for k in range(1, H):
            gx(k, c, True).start()
    for c in range(NC - XE, NC):
        for k in range(1, H):
            for q in range(1, G):
                gf(k, q, c, True).start()
    if L > 1:
        own_share(True).start()

    def gu_x(c):
        for k in range(1, H):
            gx(k, c, False).wait_recv()
            for q in range(1, G) if c < NC - XE else ():
                gy(k, q, c, True).start()
            if L > 1:
                glx(k, c, True).start()

    def gu_y(c):
        for k in range(1, H):
            for q in range(1, G):
                (gy if c < NC - XE else gf)(k, q, c, False).wait_recv()
                if L > 1:
                    gly(k, q, c, True).start()

    def meet():
        when(below, lambda: pl.semaphore_wait(s_far.at[0], 1))
        beside(above, 1, s_far.at[0])
        when(above, lambda: pl.semaphore_wait(s_far.at[1], 1))
        beside(below, -1, s_far.at[1])

    if line:
        meet()

    def dispatch():
        own_stage.wait()
        for k in range(1, N):
            da(k, False).wait_recv()
        loop(1, T, lambda k: db(k, True).start())
        mine = pltpu.make_async_copy(staged(t), down.at[t, share(d, g)], s_loc.at[2])
        mine.start()
        mine.wait()

    def down_z(k, mine):
        if not mine:
            db(k, False).wait_recv()
        for m in range(1, H):
            cx(k, m, True).start()
        for q in range(1, G):
            cy(k, 0, q, True).start()

    def down_x(k, mine=False):
        for m in range(1, H):
            cx(k, m, False).wait_recv()
            for q in () if mine else range(1, G):
                cy(k, m, q, True).start()

    def down_y(k, mine=False):
        for m in range(H):
            for q in range(1, G):
                if not mine:
                    cy(k, m, q, False).wait_recv()
                elif m:
                    cf(m, q, False).wait_recv()
            if L > 1:
                cl(k, m, True).start()

    def gu_all():
        own_gu.wait()
        if L > 1:
            own_share(False).wait_recv()
            for k in range(1, H):
                for c in range(NC):
                    glx(k, c, False).wait_recv()
                    for q in range(1, G):
                        gly(k, q, c, False).wait_recv()

    def product(b):
        at_b = pl.ds(pl.multiple_of(b * feats, 128), feats)
        return jnp.dot(tok[:, at_b], gu[b * feats // depth, pl.ds(pl.multiple_of(lax.rem(b * feats, depth), 128), feats)],
                       preferred_element_type=jnp.float32)

    def near(s, waits=False):
        def add(way):
            for c in range(TC if waits else 0):
                when(last_plane(), lambda c=c: tok_recv(way, s, c).wait_recv())
            comb[...] += product(t + s if way else t - s)

        when(t - s >= 0, lambda: add(0))
        when(t + s < T, lambda: add(1))

    def first_products():
        gu_all()
        comb[...] = product(t)
        for s in range(1, T - 1):
            near(s, True)

    def begin():
        dispatch()
        for c in range(HELD):
            tok_first(c)
        down_z(0, True)

    if T <= 8:
        own_tok.wait()
        events = [(BEGIN, begin)]
        events += [(GX + DX * c, functools.partial(gu_x, c)) for c in range(NC)]
        events += [(GY + DX * c, functools.partial(gu_y, c)) for c in range(NC)]
        events += [(PROD, first_products)]
        events += [(DZ + DDZ * (k - 1), functools.partial(down_z, nearest(k, False), False)) for k in range(1, T)]
        events += [(TOK0 if (s, c) == (1, 0) else TOK + DTOK * ((s - 1) * TC + c), functools.partial(tok_step, s, c))
                   for s in range(1, T) for c in range(TC)]
        events += [(CX + DCX * k, functools.partial(down_x, nearest(k, False) if k else 0, k == 0)) for k in range(T)]
        events += [(FAR, far_half)]
        for _, event in sorted(events, key=lambda e: e[0]):
            event()
        near(T - 1, True)
    else:
        own_tok.wait()
        for c in range(NC):
            gu_x(c)
        begin()
        for c in range(NC):
            gu_y(c)

        def whole_step(s):
            for c in range(TC):
                tok_step(s, c)

        loop(1, T, whole_step)
        loop(1, T, lambda k: down_z(k, False))
        far_half()
        down_x(0, True)
        loop(1, T, down_x)
        gu_all()
        comb[...] = product(t)
        loop(1, T, near)

    total = comb[...]
    up = pltpu.roll(total, width - 1, 1)
    wide = total / (1.0 + jnp.exp(-total)) * up
    even = lax.rem(lax.broadcasted_iota(jnp.int32, wide.shape, 1), 2) == 0
    wide = jnp.where(even, wide, 0.0).astype(jnp.bfloat16)
    pick = (lax.broadcasted_iota(jnp.int32, (width, units), 0)
            == 2 * lax.broadcasted_iota(jnp.int32, (width, units), 1))
    pick = jnp.where(pick, 1.0, 0.0).astype(jnp.bfloat16)
    hid[t] = jnp.dot(wide, pick, preferred_element_type=jnp.float32).astype(jnp.bfloat16)

    def hs(k, to):
        ref = hid.at[t if to else lax.rem(t - k + T, T)]
        return remote(ref, ref, s_hid, (k - 1,), at("tensor", lax.rem(t + k, T)))

    def shared(k):
        if L > 1:
            for m in range(H):
                cl(k, m, False).wait_recv()

    def term(k):
        tt = lax.rem(t - k + T, T)
        return jnp.dot(hid[tt], down[tt], preferred_element_type=jnp.float32)

    def mix(k):
        hs(k, False).wait_recv()
        acc[...] += term(k)

    if line:
        order = [nearest(j, True) for j in range(1, T)]
        for j in range(1, T):
            hs(lax.rem(T - nearest(T - j, False), T), True).start()
        down_y(0, True)
        for j in range(1, T):
            down_y(nearest(j, False))
        shared(0)
        acc[...] = term(0)
        for j in range(1, T - 1):
            shared(order[j - 1])
            mix(order[j - 1])
        if T > 1:
            shared(order[-1])
            hs(order[-1], False).wait_recv()
            out[...] = (acc[...] + term(order[-1])).astype(out.dtype)
        else:
            out[...] = acc[...].astype(out.dtype)
    else:
        loop(1, T, lambda k: hs(k, True).start())
        down_y(0, True)
        loop(1, T, down_y)
        loop(0, T, shared)
        acc[...] = term(0)
        loop(1, T, mix)
        out[...] = acc[...].astype(out.dtype)

    def tok_sent(s):
        for way in range(2):
            for c in range(TC):
                when(tok_can_send(way, s), lambda way=way, c=c: tok_send(way, s, c, False).wait_send())

    loop(1, T, tok_sent)
    for k in range(1, H):
        for c in range(NC):
            gx(k, c, True).wait_send()
            if L > 1:
                glx(k, c, True).wait_send()
            for q in range(1, G):
                (gy if c < NC - XE else gf)(k, q, c, True).wait_send()
                if L > 1:
                    gly(k, q, c, True).wait_send()
    if L > 1:
        own_share(True).wait_send()
    for k in range(1, N):
        da(k, True).wait_send()

    def sent(k):
        db(k, True).wait_send()
        hs(k, True).wait_send()

    loop(1, T, sent)

    def plane_sent(k, mine=False):
        for m in range(1, H):
            cx(k, m, True).wait_send()
        for m in range(H):
            for q in range(1, G):
                if mine and m:
                    cf(m, q, True).wait_send()
                else:
                    cy(k, m, q, True).wait_send()
            if L > 1:
                cl(k, m, True).wait_send()

    plane_sent(0, True)
    loop(1, T, plane_sent)


def per_device(mesh, tokens, gate_up_weight, down_weight):
    G, N, T = (mesh.shape[a] for a in ("groups", "dp", "tensor"))
    L = 2 if N % 2 == 0 else 1
    H = N // L
    NC, TC = 8, 2
    rows, feats = tokens.shape
    depth, width = gate_up_weight.shape
    units = down_weight.shape[0]
    cols = down_weight.shape[1] * N // T
    dma = pltpu.SemaphoreType.DMA
    one = max
    bf = jnp.bfloat16
    sem = lambda *shape: dma((2,) + tuple(one(1, n) for n in shape))
    return pl.pallas_call(
        functools.partial(kernel, (G, N, T, L, H, NC, TC)),
        out_shape=pltpu.VMEM((rows, cols), bf),
        in_specs=[pl.BlockSpec(memory_space=pl.ANY)] * 3,
        out_specs=pl.BlockSpec(memory_space=pltpu.VMEM),
        scratch_shapes=[
            pltpu.VMEM((rows, feats * T), bf),
            pltpu.VMEM((N, depth, width), bf),
            pltpu.VMEM((N, units // N // G, down_weight.shape[1]), bf),
            pltpu.VMEM((T, units, cols), bf),
            pltpu.VMEM((T, rows, units), bf),
            pltpu.VMEM((rows, width), jnp.float32),
            pltpu.VMEM((rows, cols), jnp.float32),
            dma((3,)),
            sem(2, T - 1, TC),
            sem(1),
            sem(H - 1, NC),
            sem(H - 1, G - 1, NC),
            sem(H - 1, NC),
            sem(H - 1, G - 1, NC),
            sem(N - 1),
            sem(T - 1),
            sem(H - 1, T),
            sem(G - 1, H, T),
            sem(H, T),
            sem(T - 1),
            sem(G - 1, H - 1),
            pltpu.SemaphoreType.REGULAR((2,)),
            sem(H - 1, G - 1, NC),
        ],
        compiler_params=pltpu.CompilerParams(collective_id=0, has_side_effects=True,
                                             vmem_limit_bytes=60 * 1024 * 1024),
    )(tokens, gate_up_weight, down_weight)


def solution(mesh):
    in_specs = (P(("groups", "dp"), "tensor"), P("dp", "tensor"), P("tensor", "dp"))
    out_specs = P(("groups", "dp"), "tensor")
    return jax.shard_map(
        functools.partial(per_device, mesh), mesh=mesh, in_specs=in_specs, out_specs=out_specs, check_vma=False
    )
```

```python
import functools

import jax
import jax.numpy as jnp
from jax import lax
from jax.experimental import pallas as pl
from jax.experimental.pallas import tpu as pltpu
from jax.sharding import PartitionSpec as P

MESH = pl.DeviceIdType.MESH
EARLY = 0
XE = 0
BEGINS, GU_X, GU_Y, PRODUCTS, DOWN_Z, DOWN_X, FAR_HALF, TOK_STEP = range(8)
ORDER = (
    (0,), (1, 0), (1, 1), (1, 2), (7, 1, 1), (7, 1, 0), (1, 3), (1, 4), (1, 5), (1, 6), (2, 0), (1, 7),
    (4, 1), (4, 2), (7, 2, 1), (5, 1), (2, 5), (4, 3), (7, 2, 0), (5, 2), (2, 2), (2, 7), (6, 0), (2, 6),
    (2, 4), (2, 1), (2, 3), (3,), (5, 3), (6, 1), (5, 0),
)
HELD = 0
FAR_SLOTS = (0, 1)


def loop(first, last, body):
    if last - first <= 8:
        for step in range(first, last):
            body(step)
    else:
        lax.fori_loop(first, last, lambda step, _: (body(step), 0)[1], 0)


def events(T, NC, TC):
    whole = [(GU_X, c) for c in range(NC)] + [(BEGINS,)] + [(GU_Y, c) for c in range(NC)]
    whole += [(TOK_STEP, s, c) for s in range(1, T) for c in range(TC)]
    whole += [(DOWN_Z, j) for j in range(1, T)] + [(FAR_HALF, j) for j in FAR_SLOTS if j < T]
    whole += [(DOWN_X, j) for j in range(T)] + [(PRODUCTS,)]
    moved = [e for e in ORDER if e in whole]
    same = set(moved) == {e for e in whole if e[0] != TOK_STEP or e[1] < T - 1}
    return moved if same else whole


def when(condition, body):
    pl.when(condition)(body)


def kernel(sizes, tok_in, gu_in, dn_in, out, tok, gu, stage, down, hid, comb, acc,
           s_loc, s_tok, s_own, s_gx, s_gy, s_glx, s_gly, s_da, s_db, s_cx, s_cy, s_cl, s_hid, s_cf, s_far, s_gf, pick):
    G, N, T, L, H, NC, TC = sizes
    g, d, t = lax.axis_index("groups"), lax.axis_index("dp"), lax.axis_index("tensor")
    hi, lo = d // L, lax.rem(d, L)
    rows, feats = tok_in.shape
    depth, width = gu_in.shape
    units, _ = dn_in.shape
    cols = out.shape[1]
    sub = dn_in.shape[1] // cols
    piece = depth // G
    chunk = piece // NC
    quarter = units // N
    part = quarter // G
    trow = rows // TC

    def at(axis, index):
        return {axis: index}

    def remote(src, dst, sem, index, device):
        return pltpu.make_async_remote_copy(
            src_ref=src, dst_ref=dst, send_sem=sem.at[(0,) + index], recv_sem=sem.at[(1,) + index],
            device_id=device, device_id_type=MESH,
        )

    def dp_of(h, l):
        return lax.rem(h + 2 * H, H) * L + l

    other = dp_of(hi, lax.rem(lo + 1, L))

    barrier = pltpu.get_barrier_semaphore()
    peers = 0
    for k in range(1, N):
        pl.semaphore_signal(barrier, inc=1, device_id=at("dp", lax.rem(d + k, N)), device_id_type=MESH)
        peers += 1
    for k in range(1, G):
        pl.semaphore_signal(barrier, inc=1, device_id=at("groups", lax.rem(g + k, G)), device_id_type=MESH)
        peers += 1

    def greet(k):
        pl.semaphore_signal(barrier, inc=1, device_id=at("tensor", lax.rem(t + k, T)), device_id_type=MESH)

    line = T <= 8
    FARS = FAR_SLOTS if line else (0,)
    below, above = t > 0, t + 1 < T

    def beside(ok, step, sem):
        when(ok, lambda: pl.semaphore_signal(sem, inc=1, device_id=at("tensor", t + step), device_id_type=MESH))

    if line:
        beside(above, 1, barrier)
        beside(below, -1, barrier)
        peers += jnp.where(below, 1, 0) + jnp.where(above, 1, 0)
    else:
        loop(1, T, greet)
        peers += T - 1

    own_tok = pltpu.make_async_copy(tok_in, tok.at[:, pl.ds(pl.multiple_of(t * feats, 128), feats)], s_loc.at[0])
    own_gu = pltpu.make_async_copy(gu_in, gu.at[d], s_loc.at[1])

    def share(dd, gg):
        return pl.ds(pl.multiple_of(dd * quarter + gg * part, 16), part)

    own_stage = pltpu.make_async_copy(dn_in.at[share(d, g)], stage.at[d], s_loc.at[2])
    own_tok.start()
    own_gu.start()
    own_stage.start()
    pl.semaphore_wait(barrier, peers)

    def nearest(j, late):
        pick = 0
        for here in range(T):
            order = sorted((p for p in range(T) if p != here),
                           key=lambda p: (late and p in (0, T - 1), abs(p - here)))
            pick = jnp.where(t == here, order[j - 1], pick)
        return lax.rem(t - pick + T, T)

    def tok_block(b, c):
        return tok.at[pl.ds(c * trow, trow), pl.ds(pl.multiple_of(b * feats, 128), feats)]

    def tok_send(way, s, c, first):
        b = t - (s - 1) if way == 0 else t + (s - 1)
        dst = tok_block(b, c)
        src = tok_in.at[pl.ds(c * trow, trow)] if first else dst
        return remote(src, dst, s_tok, (way, s - 1, c), at("tensor", t + 1 if way == 0 else t - 1))

    def tok_can_send(way, s):
        if way == 0:
            return jnp.logical_and(t + 1 < T, t - (s - 1) >= 0)
        return jnp.logical_and(t - 1 >= 0, t + (s - 1) < T)

    def tok_recv(way, s, c):
        b = t - s if way == 0 else t + s
        dst = tok_block(b, c)
        return remote(dst, dst, s_tok, (way, s - 1, c), at("tensor", t))

    def tok_has(way, s):
        return t - s >= 0 if way == 0 else t + s < T

    def last_plane():
        return jnp.logical_or(t == 0, t == T - 1)

    def tok_step(s, c):
        for way in range(2):
            def arrive(way=way):
                tok_recv(way, s, c).wait_recv()

                def forward():
                    tok_send(way, s + 1, c, False).start()

                when(tok_can_send(way, s + 1), forward)

            met = tok_has(way, s)
            when(jnp.logical_and(met, jnp.logical_not(last_plane())) if line else met, arrive)

    def gu_at(dd, gg, c):
        return gu.at[dd, pl.ds(pl.multiple_of(gg * piece + c * chunk, 16), chunk)]

    def gx(k, c, to):
        if to:
            src = gu_in.at[pl.ds(pl.multiple_of(g * piece + c * chunk, 16), chunk)]
            return remote(src, gu_at(d, g, c), s_gx, (k - 1, c), at("dp", dp_of(hi + k, lo)))
        ref = gu_at(dp_of(hi - k, lo), g, c)
        return remote(ref, ref, s_gx, (k - 1, c), at("dp", d))

    def gf(k, q, c, to):
        far = lax.rem(g - q + G, G)
        if to:
            src = gu_in.at[pl.ds(pl.multiple_of(far * piece + c * chunk, 16), chunk)]
            return remote(src, gu_at(d, far, c), s_gf, (k - 1, q - 1, c), at("dp", dp_of(hi + k, lo)))
        ref = gu_at(dp_of(hi - k, lo), far, c)
        return remote(ref, ref, s_gf, (k - 1, q - 1, c), at("dp", d))

    def gy(k, q, c, to):
        ref = gu_at(dp_of(hi - k, lo), g if to else lax.rem(g - q + G, G), c)
        return remote(ref, ref, s_gy, (k - 1, q - 1, c), at("groups", lax.rem(g + q, G)))

    def glx(k, c, to):
        ref = gu_at(dp_of(hi - k, lo if to else lax.rem(lo + 1, L)), g, c)
        return remote(ref, ref, s_glx, (k - 1, c), at("dp", other))

    def gly(k, q, c, to):
        ref = gu_at(dp_of(hi - k, lo if to else lax.rem(lo + 1, L)), lax.rem(g - q + G, G), c)
        return remote(ref, ref, s_gly, (k - 1, q - 1, c), at("dp", other))

    def own_share(to):
        return remote(gu_in, gu.at[d] if to else gu.at[other], s_own, (0,), at("dp", other))

    def da(k, to):
        if to:
            dd = lax.rem(d + k, N)
            return remote(dn_in.at[share(dd, g)], stage.at[d], s_da, (k - 1,), at("dp", dd))
        ref = stage.at[lax.rem(d - k + N, N)]
        return remote(ref, ref, s_da, (k - 1,), at("dp", d))

    def staged(tt):
        return stage.at[tt // sub, :, pl.ds(pl.multiple_of(lax.rem(tt, sub) * cols, 128), cols)]

    def db(k, to):
        tt = lax.rem(t + k, T)
        if to:
            return remote(staged(tt), down.at[t, share(d, g)], s_db, (k - 1,), at("tensor", tt))
        ref = down.at[lax.rem(t - k + T, T), share(d, g)]
        return remote(ref, ref, s_db, (k - 1,), at("tensor", t))

    def cx(k, m, to):
        tt = lax.rem(t - k + T, T)
        ref = down.at[tt, share(d if to else dp_of(hi - m, lo), g)]
        return remote(ref, ref, s_cx, (m - 1, k), at("dp", dp_of(hi + m, lo)))

    def cy(k, m, q, to):
        tt = lax.rem(t - k + T, T)
        ref = down.at[tt, share(dp_of(hi - m, lo), g if to else lax.rem(g - q + G, G))]
        return remote(ref, ref, s_cy, (q - 1, m, k), at("groups", lax.rem(g + q, G)))

    def cf(j, k, m, q, to):
        far = lax.rem(g - q + G, G)
        tt = lax.rem(t - k + T, T)
        ref = down.at[tt, share(d if to else dp_of(hi - m, lo), far)]
        return remote(ref, ref, s_cf, (q - 1, m - 1, j), at("dp", dp_of(hi + m, lo)))

    def far_half(j, k):
        for q in range(1, G):
            cy(k, 0, q, False).wait_recv()
            for m in range(1, H):
                cf(j, k, m, q, True).start()

    def cl(k, m, to):
        tt = lax.rem(t - k + T, T)
        dd = dp_of(hi - m, lo if to else lax.rem(lo + 1, L))
        ref = down.at[tt, pl.ds(pl.multiple_of(dd * quarter, 16), quarter)]
        return remote(ref, ref, s_cl, (m, k), at("dp", other))

    def tok_first(c):
        for way in range(2):
            when(tok_can_send(way, 1), lambda way=way: tok_send(way, 1, c, True).start())

    for c in range(HELD, TC):
        tok_first(c)
    for c in range(NC):
        if c == EARLY:
            for k in range(1, N):
                da(k, True).start()
        for k in range(1, H):
            gx(k, c, True).start()
    for c in range(NC - XE, NC):
        for k in range(1, H):
            for q in range(1, G):
                gf(k, q, c, True).start()
    if L > 1:
        own_share(True).start()

    def gu_x(c):
        for k in range(1, H):
            gx(k, c, False).wait_recv()
            for q in range(1, G) if c < NC - XE else ():
                gy(k, q, c, True).start()
            if L > 1:
                glx(k, c, True).start()

    def gu_y(c):
        for k in range(1, H):
            for q in range(1, G):
                (gy if c < NC - XE else gf)(k, q, c, False).wait_recv()
                if L > 1:
                    gly(k, q, c, True).start()

    def meet():
        when(below, lambda: pl.semaphore_wait(s_far.at[0], 1))
        beside(above, 1, s_far.at[0])
        when(above, lambda: pl.semaphore_wait(s_far.at[1], 1))
        beside(below, -1, s_far.at[1])

    if line:
        meet()

    chosen = (lax.broadcasted_iota(jnp.int32, (width, units), 0)
              == 2 * lax.broadcasted_iota(jnp.int32, (width, units), 1))
    pick[...] = jnp.where(chosen, 1.0, 0.0).astype(jnp.bfloat16)

    def dispatch():
        own_stage.wait()
        for k in range(1, N):
            da(k, False).wait_recv()
        loop(1, T, lambda k: db(k, True).start())
        mine = pltpu.make_async_copy(staged(t), down.at[t, share(d, g)], s_loc.at[2])
        mine.start()
        mine.wait()

    def down_z(k, mine):
        if not mine:
            db(k, False).wait_recv()
        for m in range(1, H):
            cx(k, m, True).start()
        for q in range(1, G):
            cy(k, 0, q, True).start()

    def down_x(k, j=None):
        for m in range(1, H):
            cx(k, m, False).wait_recv()
            for q in () if j in FARS else range(1, G):
                cy(k, m, q, True).start()

    def down_y(k, j=None):
        for m in range(H):
            for q in range(1, G):
                if j not in FARS:
                    cy(k, m, q, False).wait_recv()
                elif m:
                    cf(j, k, m, q, False).wait_recv()
            if L > 1:
                cl(k, m, True).start()

    def gu_all():
        own_gu.wait()
        if L > 1:
            own_share(False).wait_recv()
            for k in range(1, H):
                for c in range(NC):
                    glx(k, c, False).wait_recv()
                    for q in range(1, G):
                        gly(k, q, c, False).wait_recv()

    def product(b, part_of=slice(None)):
        at_b = pl.ds(pl.multiple_of(b * feats, 128), feats)
        return jnp.dot(tok[part_of, at_b], gu[b * feats // depth, pl.ds(pl.multiple_of(lax.rem(b * feats, depth), 128), feats)],
                       preferred_element_type=jnp.float32)

    def near(s, waits=False):
        def add(way):
            for c in range(TC if waits else 0):
                when(last_plane(), lambda c=c: tok_recv(way, s, c).wait_recv())
            comb[...] += product(t + s if way else t - s)

        when(t - s >= 0, lambda: add(0))
        when(t + s < T, lambda: add(1))

    def first_products():
        gu_all()
        comb[...] = product(t)
        for s in range(1, T - 1):
            near(s, True)

    def begin():
        dispatch()
        for c in range(HELD):
            tok_first(c)
        down_z(0, True)

    if T <= 8:
        own_tok.wait()
        slots = [0] + [nearest(j, False) for j in range(1, T)]
        steps = {
            BEGINS: begin, GU_X: gu_x, GU_Y: gu_y, PRODUCTS: first_products, TOK_STEP: tok_step,
            DOWN_Z: lambda j: down_z(slots[j], False), DOWN_X: lambda j: down_x(slots[j], j),
            FAR_HALF: lambda j: far_half(j, slots[j]),
        }
        for kind, *which in events(T, NC, TC):
            steps[kind](*which)
    else:
        own_tok.wait()
        for c in range(NC):
            gu_x(c)
        begin()
        for c in range(NC):
            gu_y(c)

        def whole_step(s):
            for c in range(TC):
                tok_step(s, c)

        loop(1, T, whole_step)
        loop(1, T, lambda k: down_z(k, False))
        far_half(0, 0)
        down_x(0, 0)
        loop(1, T, down_x)
        gu_all()
        comb[...] = product(t)
        loop(1, T, near)
    def hs(k, c, to):
        ref = hid.at[t if to else lax.rem(t - k + T, T), pl.ds(c * rows, rows)]
        return remote(ref, ref, s_hid, (k - 1, c), at("tensor", lax.rem(t + k, T)))

    def finish(c):
        total = comb[pl.ds(c * rows, rows)]
        up = pltpu.roll(total, width - 1, 1)
        wide = total / (1.0 + jnp.exp(-total)) * up
        even = lax.rem(lax.broadcasted_iota(jnp.int32, wide.shape, 1), 2) == 0
        wide = jnp.where(even, wide, 0.0).astype(jnp.bfloat16)
        hid[t, pl.ds(c * rows, rows)] = jnp.dot(
            wide, pick[...], preferred_element_type=jnp.float32).astype(jnp.bfloat16)

    def last_rows(way, c):
        for p in range(TC):
            tok_recv(way, T - 1, p).wait_recv()
        part_of = pl.ds(c * rows, rows)
        comb[part_of] += product(t + T - 1 if way else t - T + 1, part_of)

    for c in range(1):
        if line and T > 1:
            when(t == T - 1, lambda c=c: last_rows(0, c))
            when(t == 0, lambda c=c: last_rows(1, c))
        finish(c)
        if line:
            for j in range(1, T):
                hs(lax.rem(T - nearest(T - j, False), T), c, True).start()
        else:
            loop(1, T, lambda k, c=c: hs(k, c, True).start())

    def shared(k):
        if L > 1:
            for m in range(H):
                cl(k, m, False).wait_recv()

    def term(k):
        tt = lax.rem(t - k + T, T)
        return jnp.dot(hid[tt], down[tt], preferred_element_type=jnp.float32)

    def mix(k):
        for c in range(1):
            hs(k, c, False).wait_recv()
        acc[...] += term(k)

    if line:
        order = [nearest(j, True) for j in range(1, T)]
        for j in range(T):
            down_y(slots[j], j)
        shared(0)
        acc[...] = term(0)
        for j in range(1, T - 1):
            shared(order[j - 1])
            mix(order[j - 1])
        if T > 1:
            shared(order[-1])
            for c in range(1):
                hs(order[-1], c, False).wait_recv()
            out[...] = (acc[...] + term(order[-1])).astype(out.dtype)
        else:
            out[...] = acc[...].astype(out.dtype)
    else:
        down_y(0, 0)
        loop(1, T, down_y)
        loop(0, T, shared)
        acc[...] = term(0)
        loop(1, T, mix)
        out[...] = acc[...].astype(out.dtype)

    def tok_sent(s):
        for way in range(2):
            for c in range(TC):
                when(tok_can_send(way, s), lambda way=way, c=c: tok_send(way, s, c, False).wait_send())

    loop(1, T, tok_sent)
    for k in range(1, H):
        for c in range(NC):
            gx(k, c, True).wait_send()
            if L > 1:
                glx(k, c, True).wait_send()
            for q in range(1, G):
                (gy if c < NC - XE else gf)(k, q, c, True).wait_send()
                if L > 1:
                    gly(k, q, c, True).wait_send()
    if L > 1:
        own_share(True).wait_send()
    for k in range(1, N):
        da(k, True).wait_send()

    def sent(k):
        db(k, True).wait_send()
        for c in range(1):
            hs(k, c, True).wait_send()

    loop(1, T, sent)

    def plane_sent(k, j=None):
        for m in range(1, H):
            cx(k, m, True).wait_send()
        for m in range(H):
            for q in range(1, G):
                if j in FARS and m:
                    cf(j, k, m, q, True).wait_send()
                else:
                    cy(k, m, q, True).wait_send()
            if L > 1:
                cl(k, m, True).wait_send()

    if line:
        for j in range(T):
            plane_sent(slots[j], j)
    else:
        plane_sent(0, 0)
        loop(1, T, plane_sent)


def per_device(mesh, tokens, gate_up_weight, down_weight):
    G, N, T = (mesh.shape[a] for a in ("groups", "dp", "tensor"))
    L = 2 if N % 2 == 0 else 1
    H = N // L
    NC, TC = 8, 2
    rows, feats = tokens.shape
    depth, width = gate_up_weight.shape
    units = down_weight.shape[0]
    cols = down_weight.shape[1] * N // T
    dma = pltpu.SemaphoreType.DMA
    one = max
    bf = jnp.bfloat16
    sem = lambda *shape: dma((2,) + tuple(one(1, n) for n in shape))
    return pl.pallas_call(
        functools.partial(kernel, (G, N, T, L, H, NC, TC)),
        out_shape=pltpu.VMEM((rows, cols), bf),
        in_specs=[pl.BlockSpec(memory_space=pl.ANY)] * 3,
        out_specs=pl.BlockSpec(memory_space=pltpu.VMEM),
        scratch_shapes=[
            pltpu.VMEM((rows, feats * T), bf),
            pltpu.VMEM((N, depth, width), bf),
            pltpu.VMEM((N, units // N // G, down_weight.shape[1]), bf),
            pltpu.VMEM((T, units, cols), bf),
            pltpu.VMEM((T, rows, units), bf),
            pltpu.VMEM((rows, width), jnp.float32),
            pltpu.VMEM((rows, cols), jnp.float32),
            dma((3,)),
            sem(2, T - 1, TC),
            sem(1),
            sem(H - 1, NC),
            sem(H - 1, G - 1, NC),
            sem(H - 1, NC),
            sem(H - 1, G - 1, NC),
            sem(N - 1),
            sem(T - 1),
            sem(H - 1, T),
            sem(G - 1, H, T),
            sem(H, T),
            sem(T - 1, TC),
            sem(G - 1, H - 1, T),
            pltpu.SemaphoreType.REGULAR((2,)),
            sem(H - 1, G - 1, NC),
            pltpu.VMEM((width, units), bf),
        ],
        compiler_params=pltpu.CompilerParams(collective_id=0, has_side_effects=True,
                                             vmem_limit_bytes=60 * 1024 * 1024),
    )(tokens, gate_up_weight, down_weight)


def solution(mesh):
    in_specs = (P(("groups", "dp"), "tensor"), P("dp", "tensor"), P("tensor", "dp"))
    out_specs = P(("groups", "dp"), "tensor")
    return jax.shard_map(
        functools.partial(per_device, mesh), mesh=mesh, in_specs=in_specs, out_specs=out_specs, check_vma=False
    )
```

```python
import functools

import jax
import jax.numpy as jnp
from jax import lax
from jax.experimental import pallas as pl
from jax.experimental.pallas import tpu as pltpu
from jax.sharding import PartitionSpec as P

MESH = pl.DeviceIdType.MESH
EARLY = 0
XE = 0
HELD = 0
BEGINS, GU_X, GU_Y, PRODUCTS, DOWN_Z, DOWN_X, FAR_HALF, TOK_STEP = range(8)
ORDERS = (
    (
        (0,), (1, 0), (1, 1), (1, 2), (1, 3), (1, 4), (1, 5), (1, 6), (2, 0), (1, 7), (4, 1), (4, 2), (2, 5),
        (4, 3), (2, 7), (2, 4), (5, 1), (5, 2), (2, 2), (6, 0), (2, 6), (2, 1), (2, 3), (3,), (5, 3), (6, 1),
        (5, 0),
    ),
    (
        (0,), (1, 0), (1, 1), (1, 2), (7, 1, 1), (7, 1, 0), (1, 3), (1, 4), (1, 5), (1, 6), (2, 0), (1, 7),
        (4, 1), (4, 2), (7, 2, 1), (2, 5), (4, 3), (7, 2, 0), (2, 7), (5, 1), (2, 4), (5, 2), (6, 0), (2, 6),
        (2, 2), (2, 1), (2, 3), (3,), (5, 3), (6, 1), (5, 0),
    ),
)
FAR_SLOTS = (0, 1)


def loop(first, last, body):
    if last - first <= 8:
        for step in range(first, last):
            body(step)
    else:
        lax.fori_loop(first, last, lambda step, _: (body(step), 0)[1], 0)


def events(T, NC, TC):
    whole = [(GU_X, c) for c in range(NC)] + [(BEGINS,)] + [(GU_Y, c) for c in range(NC)]
    tokens = [(TOK_STEP, s, c) for s in range(1, T) for c in range(TC)]
    rest = [(DOWN_Z, j) for j in range(1, T)] + [(FAR_HALF, j) for j in FAR_SLOTS if j < T]
    rest += [(DOWN_X, j) for j in range(T)] + [(PRODUCTS,)]
    used = [e for e in tokens if e[1] < T - 1]
    plain = (whole + rest, whole + used + rest)
    same = all(sorted(a) == sorted(b) for a, b in zip(ORDERS, plain))
    return ORDERS if same else plain


def when(condition, body):
    pl.when(condition)(body)


def kernel(sizes, tok_in, gu_in, dn_in, out, tok, gu, stage, down, hid, comb, acc,
           s_loc, s_tok, s_own, s_gx, s_gy, s_glx, s_gly, s_da, s_db, s_cx, s_cy, s_cl, s_hid, s_cf, s_far, s_gf, pick):
    G, N, T, L, H, NC, TC = sizes
    g, d, t = lax.axis_index("groups"), lax.axis_index("dp"), lax.axis_index("tensor")
    hi, lo = d // L, lax.rem(d, L)
    rows, feats = tok_in.shape
    depth, width = gu_in.shape
    units, _ = dn_in.shape
    cols = out.shape[1]
    sub = dn_in.shape[1] // cols
    piece = depth // G
    chunk = piece // NC
    quarter = units // N
    part = quarter // G
    trow = rows // TC

    def at(axis, index):
        return {axis: index}

    def remote(src, dst, sem, index, device):
        return pltpu.make_async_remote_copy(
            src_ref=src, dst_ref=dst, send_sem=sem.at[(0,) + index], recv_sem=sem.at[(1,) + index],
            device_id=device, device_id_type=MESH,
        )

    def dp_of(h, l):
        return lax.rem(h + 2 * H, H) * L + l

    other = dp_of(hi, lax.rem(lo + 1, L))

    barrier = pltpu.get_barrier_semaphore()
    peers = 0
    for k in range(1, N):
        pl.semaphore_signal(barrier, inc=1, device_id=at("dp", lax.rem(d + k, N)), device_id_type=MESH)
        peers += 1
    for k in range(1, G):
        pl.semaphore_signal(barrier, inc=1, device_id=at("groups", lax.rem(g + k, G)), device_id_type=MESH)
        peers += 1

    def greet(k):
        pl.semaphore_signal(barrier, inc=1, device_id=at("tensor", lax.rem(t + k, T)), device_id_type=MESH)

    line = T <= 8
    FARS = FAR_SLOTS if line else (0,)
    below, above = t > 0, t + 1 < T

    def beside(ok, step, sem):
        when(ok, lambda: pl.semaphore_signal(sem, inc=1, device_id=at("tensor", t + step), device_id_type=MESH))

    if line:
        beside(above, 1, barrier)
        beside(below, -1, barrier)
        peers += jnp.where(below, 1, 0) + jnp.where(above, 1, 0)
    else:
        loop(1, T, greet)
        peers += T - 1

    own_tok = pltpu.make_async_copy(tok_in, tok.at[:, pl.ds(pl.multiple_of(t * feats, 128), feats)], s_loc.at[0])
    own_gu = pltpu.make_async_copy(gu_in, gu.at[d], s_loc.at[1])

    def share(dd, gg):
        return pl.ds(pl.multiple_of(dd * quarter + gg * part, 16), part)

    own_stage = pltpu.make_async_copy(dn_in.at[share(d, g)], stage.at[d], s_loc.at[2])
    own_tok.start()
    own_gu.start()
    own_stage.start()
    pl.semaphore_wait(barrier, peers)

    def nearest(j, late):
        pick = 0
        for here in range(T):
            order = sorted((p for p in range(T) if p != here),
                           key=lambda p: (late and p in (0, T - 1), abs(p - here)))
            pick = jnp.where(t == here, order[j - 1], pick)
        return lax.rem(t - pick + T, T)

    def tok_block(b, c):
        return tok.at[pl.ds(c * trow, trow), pl.ds(pl.multiple_of(b * feats, 128), feats)]

    def tok_send(way, s, c, first):
        b = t - (s - 1) if way == 0 else t + (s - 1)
        dst = tok_block(b, c)
        src = tok_in.at[pl.ds(c * trow, trow)] if first else dst
        return remote(src, dst, s_tok, (way, s - 1, c), at("tensor", t + 1 if way == 0 else t - 1))

    def tok_can_send(way, s):
        if way == 0:
            return jnp.logical_and(t + 1 < T, t - (s - 1) >= 0)
        return jnp.logical_and(t - 1 >= 0, t + (s - 1) < T)

    def tok_recv(way, s, c):
        b = t - s if way == 0 else t + s
        dst = tok_block(b, c)
        return remote(dst, dst, s_tok, (way, s - 1, c), at("tensor", t))

    def tok_has(way, s):
        return t - s >= 0 if way == 0 else t + s < T

    def last_plane():
        return jnp.logical_or(t == 0, t == T - 1)

    def tok_step(s, c):
        for way in range(2):
            def arrive(way=way):
                tok_recv(way, s, c).wait_recv()

                def forward():
                    tok_send(way, s + 1, c, False).start()

                when(tok_can_send(way, s + 1), forward)

            met = tok_has(way, s)
            when(jnp.logical_and(met, jnp.logical_not(last_plane())) if line else met, arrive)

    def gu_at(dd, gg, c):
        return gu.at[dd, pl.ds(pl.multiple_of(gg * piece + c * chunk, 16), chunk)]

    def gx(k, c, to):
        if to:
            src = gu_in.at[pl.ds(pl.multiple_of(g * piece + c * chunk, 16), chunk)]
            return remote(src, gu_at(d, g, c), s_gx, (k - 1, c), at("dp", dp_of(hi + k, lo)))
        ref = gu_at(dp_of(hi - k, lo), g, c)
        return remote(ref, ref, s_gx, (k - 1, c), at("dp", d))

    def gf(k, q, c, to):
        far = lax.rem(g - q + G, G)
        if to:
            src = gu_in.at[pl.ds(pl.multiple_of(far * piece + c * chunk, 16), chunk)]
            return remote(src, gu_at(d, far, c), s_gf, (k - 1, q - 1, c), at("dp", dp_of(hi + k, lo)))
        ref = gu_at(dp_of(hi - k, lo), far, c)
        return remote(ref, ref, s_gf, (k - 1, q - 1, c), at("dp", d))

    def gy(k, q, c, to):
        ref = gu_at(dp_of(hi - k, lo), g if to else lax.rem(g - q + G, G), c)
        return remote(ref, ref, s_gy, (k - 1, q - 1, c), at("groups", lax.rem(g + q, G)))

    def glx(k, c, to):
        ref = gu_at(dp_of(hi - k, lo if to else lax.rem(lo + 1, L)), g, c)
        return remote(ref, ref, s_glx, (k - 1, c), at("dp", other))

    def gly(k, q, c, to):
        ref = gu_at(dp_of(hi - k, lo if to else lax.rem(lo + 1, L)), lax.rem(g - q + G, G), c)
        return remote(ref, ref, s_gly, (k - 1, q - 1, c), at("dp", other))

    def own_share(to):
        return remote(gu_in, gu.at[d] if to else gu.at[other], s_own, (0,), at("dp", other))

    def da(k, to):
        if to:
            dd = lax.rem(d + k, N)
            return remote(dn_in.at[share(dd, g)], stage.at[d], s_da, (k - 1,), at("dp", dd))
        ref = stage.at[lax.rem(d - k + N, N)]
        return remote(ref, ref, s_da, (k - 1,), at("dp", d))

    def staged(tt):
        return stage.at[tt // sub, :, pl.ds(pl.multiple_of(lax.rem(tt, sub) * cols, 128), cols)]

    def db(k, to):
        tt = lax.rem(t + k, T)
        if to:
            return remote(staged(tt), down.at[t, share(d, g)], s_db, (k - 1,), at("tensor", tt))
        ref = down.at[lax.rem(t - k + T, T), share(d, g)]
        return remote(ref, ref, s_db, (k - 1,), at("tensor", t))

    def cx(k, m, to):
        tt = lax.rem(t - k + T, T)
        ref = down.at[tt, share(d if to else dp_of(hi - m, lo), g)]
        return remote(ref, ref, s_cx, (m - 1, k), at("dp", dp_of(hi + m, lo)))

    def cy(k, m, q, to):
        tt = lax.rem(t - k + T, T)
        ref = down.at[tt, share(dp_of(hi - m, lo), g if to else lax.rem(g - q + G, G))]
        return remote(ref, ref, s_cy, (q - 1, m, k), at("groups", lax.rem(g + q, G)))

    def cf(j, k, m, q, to):
        far = lax.rem(g - q + G, G)
        tt = lax.rem(t - k + T, T)
        ref = down.at[tt, share(d if to else dp_of(hi - m, lo), far)]
        return remote(ref, ref, s_cf, (q - 1, m - 1, j), at("dp", dp_of(hi + m, lo)))

    def far_half(j, k):
        for q in range(1, G):
            cy(k, 0, q, False).wait_recv()
            for m in range(1, H):
                cf(j, k, m, q, True).start()

    def cl(k, m, to):
        tt = lax.rem(t - k + T, T)
        dd = dp_of(hi - m, lo if to else lax.rem(lo + 1, L))
        ref = down.at[tt, pl.ds(pl.multiple_of(dd * quarter, 16), quarter)]
        return remote(ref, ref, s_cl, (m, k), at("dp", other))

    def tok_first(c):
        for way in range(2):
            when(tok_can_send(way, 1), lambda way=way: tok_send(way, 1, c, True).start())

    for c in range(HELD, TC):
        tok_first(c)
    for c in range(NC):
        if c == EARLY:
            for k in range(1, N):
                da(k, True).start()
        for k in range(1, H):
            gx(k, c, True).start()
    for c in range(NC - XE, NC):
        for k in range(1, H):
            for q in range(1, G):
                gf(k, q, c, True).start()
    if L > 1:
        own_share(True).start()

    def gu_x(c):
        for k in range(1, H):
            gx(k, c, False).wait_recv()
            for q in range(1, G) if c < NC - XE else ():
                gy(k, q, c, True).start()
            if L > 1:
                glx(k, c, True).start()

    def gu_y(c):
        for k in range(1, H):
            for q in range(1, G):
                (gy if c < NC - XE else gf)(k, q, c, False).wait_recv()
                if L > 1:
                    gly(k, q, c, True).start()

    def meet():
        when(below, lambda: pl.semaphore_wait(s_far.at[0], 1))
        beside(above, 1, s_far.at[0])
        when(above, lambda: pl.semaphore_wait(s_far.at[1], 1))
        beside(below, -1, s_far.at[1])

    if line:
        meet()

    chosen = (lax.broadcasted_iota(jnp.int32, (width, units), 0)
              == 2 * lax.broadcasted_iota(jnp.int32, (width, units), 1))
    pick[...] = jnp.where(chosen, 1.0, 0.0).astype(jnp.bfloat16)

    def dispatch():
        own_stage.wait()
        for k in range(1, N):
            da(k, False).wait_recv()
        loop(1, T, lambda k: db(k, True).start())
        mine = pltpu.make_async_copy(staged(t), down.at[t, share(d, g)], s_loc.at[2])
        mine.start()
        mine.wait()

    def down_z(k, mine):
        if not mine:
            db(k, False).wait_recv()
        for m in range(1, H):
            cx(k, m, True).start()
        for q in range(1, G):
            cy(k, 0, q, True).start()

    def down_x(k, j=None):
        for m in range(1, H):
            cx(k, m, False).wait_recv()
            for q in () if j in FARS else range(1, G):
                cy(k, m, q, True).start()

    def down_y(k, j=None):
        for m in range(H):
            for q in range(1, G):
                if j not in FARS:
                    cy(k, m, q, False).wait_recv()
                elif m:
                    cf(j, k, m, q, False).wait_recv()
            if L > 1:
                cl(k, m, True).start()

    def gu_all():
        own_gu.wait()
        if L > 1:
            own_share(False).wait_recv()
            for k in range(1, H):
                for c in range(NC):
                    glx(k, c, False).wait_recv()
                    for q in range(1, G):
                        gly(k, q, c, False).wait_recv()

    def product(b, part_of=slice(None)):
        at_b = pl.ds(pl.multiple_of(b * feats, 128), feats)
        return jnp.dot(tok[part_of, at_b], gu[b * feats // depth, pl.ds(pl.multiple_of(lax.rem(b * feats, depth), 128), feats)],
                       preferred_element_type=jnp.float32)

    def near(s, waits=False):
        def add(way):
            for c in range(TC if waits else 0):
                when(last_plane(), lambda c=c: tok_recv(way, s, c).wait_recv())
            comb[...] += product(t + s if way else t - s)

        when(t - s >= 0, lambda: add(0))
        when(t + s < T, lambda: add(1))

    def first_products():
        gu_all()
        comb[...] = product(t)
        for s in range(1, T - 1):
            near(s, True)

    def begin():
        dispatch()
        for c in range(HELD):
            tok_first(c)
        down_z(0, True)

    if T <= 8:
        own_tok.wait()
        slots = [0] + [nearest(j, False) for j in range(1, T)]
        steps = {
            BEGINS: begin, GU_X: gu_x, GU_Y: gu_y, PRODUCTS: first_products, TOK_STEP: tok_step,
            DOWN_Z: lambda j: down_z(slots[j], False), DOWN_X: lambda j: down_x(slots[j], j),
            FAR_HALF: lambda j: far_half(j, slots[j]),
        }

        def run(order):
            for kind, *which in order:
                steps[kind](*which)

        ends, others = events(T, NC, TC)
        when(last_plane(), lambda: run(ends))
        when(jnp.logical_not(last_plane()), lambda: run(others))
    else:
        own_tok.wait()
        for c in range(NC):
            gu_x(c)
        begin()
        for c in range(NC):
            gu_y(c)

        def whole_step(s):
            for c in range(TC):
                tok_step(s, c)

        loop(1, T, whole_step)
        loop(1, T, lambda k: down_z(k, False))
        far_half(0, 0)
        down_x(0, 0)
        loop(1, T, down_x)
        gu_all()
        comb[...] = product(t)
        loop(1, T, near)
    def hs(k, c, to):
        ref = hid.at[t if to else lax.rem(t - k + T, T), pl.ds(c * rows, rows)]
        return remote(ref, ref, s_hid, (k - 1, c), at("tensor", lax.rem(t + k, T)))

    def finish(c):
        total = comb[pl.ds(c * rows, rows)]
        up = pltpu.roll(total, width - 1, 1)
        wide = total / (1.0 + jnp.exp(-total)) * up
        even = lax.rem(lax.broadcasted_iota(jnp.int32, wide.shape, 1), 2) == 0
        wide = jnp.where(even, wide, 0.0).astype(jnp.bfloat16)
        hid[t, pl.ds(c * rows, rows)] = jnp.dot(
            wide, pick[...], preferred_element_type=jnp.float32).astype(jnp.bfloat16)

    def last_rows(way, c):
        for p in range(TC):
            tok_recv(way, T - 1, p).wait_recv()
        part_of = pl.ds(c * rows, rows)
        comb[part_of] += product(t + T - 1 if way else t - T + 1, part_of)

    for c in range(1):
        if line and T > 1:
            when(t == T - 1, lambda c=c: last_rows(0, c))
            when(t == 0, lambda c=c: last_rows(1, c))
        finish(c)
        if line:
            for j in range(1, T):
                hs(lax.rem(T - nearest(T - j, False), T), c, True).start()
        else:
            loop(1, T, lambda k, c=c: hs(k, c, True).start())

    def shared(k):
        if L > 1:
            for m in range(H):
                cl(k, m, False).wait_recv()

    def term(k):
        tt = lax.rem(t - k + T, T)
        return jnp.dot(hid[tt], down[tt], preferred_element_type=jnp.float32)

    def mix(k):
        for c in range(1):
            hs(k, c, False).wait_recv()
        acc[...] += term(k)

    if line:
        order = [nearest(j, True) for j in range(1, T)]
        for j in range(T):
            down_y(slots[j], j)
        shared(0)
        acc[...] = term(0)
        for j in range(1, T - 1):
            shared(order[j - 1])
            mix(order[j - 1])
        if T > 1:
            shared(order[-1])
            for c in range(1):
                hs(order[-1], c, False).wait_recv()
            out[...] = (acc[...] + term(order[-1])).astype(out.dtype)
        else:
            out[...] = acc[...].astype(out.dtype)
    else:
        down_y(0, 0)
        loop(1, T, down_y)
        loop(0, T, shared)
        acc[...] = term(0)
        loop(1, T, mix)
        out[...] = acc[...].astype(out.dtype)

    def tok_sent(s):
        for way in range(2):
            for c in range(TC):
                when(tok_can_send(way, s), lambda way=way, c=c: tok_send(way, s, c, False).wait_send())

    loop(1, T, tok_sent)
    for k in range(1, H):
        for c in range(NC):
            gx(k, c, True).wait_send()
            if L > 1:
                glx(k, c, True).wait_send()
            for q in range(1, G):
                (gy if c < NC - XE else gf)(k, q, c, True).wait_send()
                if L > 1:
                    gly(k, q, c, True).wait_send()
    if L > 1:
        own_share(True).wait_send()
    for k in range(1, N):
        da(k, True).wait_send()

    def sent(k):
        db(k, True).wait_send()
        for c in range(1):
            hs(k, c, True).wait_send()

    loop(1, T, sent)

    def plane_sent(k, j=None):
        for m in range(1, H):
            cx(k, m, True).wait_send()
        for m in range(H):
            for q in range(1, G):
                if j in FARS and m:
                    cf(j, k, m, q, True).wait_send()
                else:
                    cy(k, m, q, True).wait_send()
            if L > 1:
                cl(k, m, True).wait_send()

    if line:
        for j in range(T):
            plane_sent(slots[j], j)
    else:
        plane_sent(0, 0)
        loop(1, T, plane_sent)


def per_device(mesh, tokens, gate_up_weight, down_weight):
    G, N, T = (mesh.shape[a] for a in ("groups", "dp", "tensor"))
    L = 2 if N % 2 == 0 else 1
    H = N // L
    NC, TC = 8, 2
    rows, feats = tokens.shape
    depth, width = gate_up_weight.shape
    units = down_weight.shape[0]
    cols = down_weight.shape[1] * N // T
    dma = pltpu.SemaphoreType.DMA
    one = max
    bf = jnp.bfloat16
    sem = lambda *shape: dma((2,) + tuple(one(1, n) for n in shape))
    return pl.pallas_call(
        functools.partial(kernel, (G, N, T, L, H, NC, TC)),
        out_shape=pltpu.VMEM((rows, cols), bf),
        in_specs=[pl.BlockSpec(memory_space=pl.ANY)] * 3,
        out_specs=pl.BlockSpec(memory_space=pltpu.VMEM),
        scratch_shapes=[
            pltpu.VMEM((rows, feats * T), bf),
            pltpu.VMEM((N, depth, width), bf),
            pltpu.VMEM((N, units // N // G, down_weight.shape[1]), bf),
            pltpu.VMEM((T, units, cols), bf),
            pltpu.VMEM((T, rows, units), bf),
            pltpu.VMEM((rows, width), jnp.float32),
            pltpu.VMEM((rows, cols), jnp.float32),
            dma((3,)),
            sem(2, T - 1, TC),
            sem(1),
            sem(H - 1, NC),
            sem(H - 1, G - 1, NC),
            sem(H - 1, NC),
            sem(H - 1, G - 1, NC),
            sem(N - 1),
            sem(T - 1),
            sem(H - 1, T),
            sem(G - 1, H, T),
            sem(H, T),
            sem(T - 1, TC),
            sem(G - 1, H - 1, T),
            pltpu.SemaphoreType.REGULAR((2,)),
            sem(H - 1, G - 1, NC),
            pltpu.VMEM((width, units), bf),
        ],
        compiler_params=pltpu.CompilerParams(collective_id=0, has_side_effects=True,
                                             vmem_limit_bytes=60 * 1024 * 1024),
    )(tokens, gate_up_weight, down_weight)


def solution(mesh):
    in_specs = (P(("groups", "dp"), "tensor"), P("dp", "tensor"), P("tensor", "dp"))
    out_specs = P(("groups", "dp"), "tensor")
    return jax.shard_map(
        functools.partial(per_device, mesh), mesh=mesh, in_specs=in_specs, out_specs=out_specs, check_vma=False
    )
```

```python
import functools

import jax
import jax.numpy as jnp
from jax import lax
from jax.experimental import pallas as pl
from jax.experimental.pallas import tpu as pltpu
from jax.sharding import PartitionSpec as P

MESH = pl.DeviceIdType.MESH
EARLY = 0
XE = 0
HELD = 0
BEGINS, GU_X, GU_Y, PRODUCTS, DOWN_Z, DOWN_X, FAR_HALF, TOK_STEP = range(8)
ORDERS = (
    (
        (0,), (1, 0), (1, 1), (1, 2), (1, 3), (1, 4), (1, 5), (1, 6), (2, 0), (1, 7), (4, 1), (4, 2), (2, 5),
        (4, 3), (2, 7), (2, 4), (5, 1), (5, 2), (2, 2), (6, 0), (2, 6), (2, 1), (2, 3), (3,), (5, 3), (6, 1),
        (5, 0),
    ),
    (
        (0,), (1, 0), (1, 1), (1, 2), (7, 1, 1), (7, 1, 0), (1, 3), (1, 4), (1, 5), (1, 6), (2, 0), (1, 7),
        (4, 1), (4, 2), (7, 2, 1), (2, 5), (4, 3), (7, 2, 0), (2, 7), (5, 1), (2, 4), (5, 2), (6, 0), (2, 6),
        (2, 2), (2, 1), (2, 3), (3,), (5, 3), (6, 1), (5, 0),
    ),
)
FAR_SLOTS = (0, 1)


def loop(first, last, body):
    if last - first <= 8:
        for step in range(first, last):
            body(step)
    else:
        lax.fori_loop(first, last, lambda step, _: (body(step), 0)[1], 0)


def events(T, NC, TC):
    whole = [(GU_X, c) for c in range(NC)] + [(BEGINS,)] + [(GU_Y, c) for c in range(NC)]
    tokens = [(TOK_STEP, s, c) for s in range(1, T) for c in range(TC)]
    rest = [(DOWN_Z, j) for j in range(1, T)] + [(FAR_HALF, j) for j in FAR_SLOTS if j < T]
    rest += [(DOWN_X, j) for j in range(T)] + [(PRODUCTS,)]
    used = [e for e in tokens if e[1] < T - 1]
    plain = (whole + rest, whole + used + rest)
    same = all(sorted(a) == sorted(b) for a, b in zip(ORDERS, plain))
    return ORDERS if same else plain


def when(condition, body):
    pl.when(condition)(body)


def kernel(sizes, tok_in, gu_in, dn_in, out, tok, gu, stage, down, hid, comb, acc,
           s_loc, s_tok, s_own, s_gx, s_gy, s_glx, s_gly, s_da, s_db, s_cx, s_cy, s_cl, s_hid, s_cf, s_far, s_gf, pick):
    G, N, T, L, H, NC, TC = sizes
    g, d, t = lax.axis_index("groups"), lax.axis_index("dp"), lax.axis_index("tensor")
    hi, lo = d // L, lax.rem(d, L)
    rows, feats = tok_in.shape
    depth, width = gu_in.shape
    units, _ = dn_in.shape
    cols = out.shape[1]
    sub = dn_in.shape[1] // cols
    piece = depth // G
    chunk = piece // NC
    quarter = units // N
    part = quarter // G
    trow = rows // TC

    def at(axis, index):
        return {axis: index}

    def remote(src, dst, sem, index, device):
        return pltpu.make_async_remote_copy(
            src_ref=src, dst_ref=dst, send_sem=sem.at[(0,) + index], recv_sem=sem.at[(1,) + index],
            device_id=device, device_id_type=MESH,
        )

    def dp_of(h, l):
        return lax.rem(h + 2 * H, H) * L + l

    other = dp_of(hi, lax.rem(lo + 1, L))

    barrier = pltpu.get_barrier_semaphore()
    peers = 0
    for k in range(1, N):
        pl.semaphore_signal(barrier, inc=1, device_id=at("dp", lax.rem(d + k, N)), device_id_type=MESH)
        peers += 1
    for k in range(1, G):
        pl.semaphore_signal(barrier, inc=1, device_id=at("groups", lax.rem(g + k, G)), device_id_type=MESH)
        peers += 1

    def greet(k):
        pl.semaphore_signal(barrier, inc=1, device_id=at("tensor", lax.rem(t + k, T)), device_id_type=MESH)

    line = T <= 8
    FARS = FAR_SLOTS if line else (0,)
    below, above = t > 0, t + 1 < T

    def beside(ok, step, sem):
        when(ok, lambda: pl.semaphore_signal(sem, inc=1, device_id=at("tensor", t + step), device_id_type=MESH))

    if line:
        beside(above, 1, barrier)
        beside(below, -1, barrier)
        peers += jnp.where(below, 1, 0) + jnp.where(above, 1, 0)
    else:
        loop(1, T, greet)
        peers += T - 1

    own_tok = pltpu.make_async_copy(tok_in, tok.at[:, pl.ds(pl.multiple_of(t * feats, 128), feats)], s_loc.at[0])
    own_gu = pltpu.make_async_copy(gu_in, gu.at[d], s_loc.at[1])

    def share(dd, gg):
        return pl.ds(pl.multiple_of(dd * quarter + gg * part, 16), part)

    own_stage = pltpu.make_async_copy(dn_in.at[share(d, g)], stage.at[d], s_loc.at[2])
    own_tok.start()
    own_gu.start()
    own_stage.start()
    pl.semaphore_wait(barrier, peers)

    def nearest(j, late):
        pick = 0
        for here in range(T):
            order = sorted((p for p in range(T) if p != here),
                           key=lambda p: (late and p in (0, T - 1), abs(p - here), -abs(2 * p - T + 1)))
            pick = jnp.where(t == here, order[j - 1], pick)
        return lax.rem(t - pick + T, T)

    def tok_block(b, c):
        return tok.at[pl.ds(c * trow, trow), pl.ds(pl.multiple_of(b * feats, 128), feats)]

    def tok_send(way, s, c, first):
        b = t - (s - 1) if way == 0 else t + (s - 1)
        dst = tok_block(b, c)
        src = tok_in.at[pl.ds(c * trow, trow)] if first else dst
        return remote(src, dst, s_tok, (way, s - 1, c), at("tensor", t + 1 if way == 0 else t - 1))

    def tok_can_send(way, s):
        if way == 0:
            return jnp.logical_and(t + 1 < T, t - (s - 1) >= 0)
        return jnp.logical_and(t - 1 >= 0, t + (s - 1) < T)

    def tok_recv(way, s, c):
        b = t - s if way == 0 else t + s
        dst = tok_block(b, c)
        return remote(dst, dst, s_tok, (way, s - 1, c), at("tensor", t))

    def tok_has(way, s):
        return t - s >= 0 if way == 0 else t + s < T

    def last_plane():
        return jnp.logical_or(t == 0, t == T - 1)

    def tok_step(s, c):
        for way in range(2):
            def arrive(way=way):
                tok_recv(way, s, c).wait_recv()

                def forward():
                    tok_send(way, s + 1, c, False).start()

                when(tok_can_send(way, s + 1), forward)

            met = tok_has(way, s)
            when(jnp.logical_and(met, jnp.logical_not(last_plane())) if line else met, arrive)

    def gu_at(dd, gg, c):
        return gu.at[dd, pl.ds(pl.multiple_of(gg * piece + c * chunk, 16), chunk)]

    def gx(k, c, to):
        if to:
            src = gu_in.at[pl.ds(pl.multiple_of(g * piece + c * chunk, 16), chunk)]
            return remote(src, gu_at(d, g, c), s_gx, (k - 1, c), at("dp", dp_of(hi + k, lo)))
        ref = gu_at(dp_of(hi - k, lo), g, c)
        return remote(ref, ref, s_gx, (k - 1, c), at("dp", d))

    def gf(k, q, c, to):
        far = lax.rem(g - q + G, G)
        if to:
            src = gu_in.at[pl.ds(pl.multiple_of(far * piece + c * chunk, 16), chunk)]
            return remote(src, gu_at(d, far, c), s_gf, (k - 1, q - 1, c), at("dp", dp_of(hi + k, lo)))
        ref = gu_at(dp_of(hi - k, lo), far, c)
        return remote(ref, ref, s_gf, (k - 1, q - 1, c), at("dp", d))

    def gy(k, q, c, to):
        ref = gu_at(dp_of(hi - k, lo), g if to else lax.rem(g - q + G, G), c)
        return remote(ref, ref, s_gy, (k - 1, q - 1, c), at("groups", lax.rem(g + q, G)))

    def glx(k, c, to):
        ref = gu_at(dp_of(hi - k, lo if to else lax.rem(lo + 1, L)), g, c)
        return remote(ref, ref, s_glx, (k - 1, c), at("dp", other))

    def gly(k, q, c, to):
        ref = gu_at(dp_of(hi - k, lo if to else lax.rem(lo + 1, L)), lax.rem(g - q + G, G), c)
        return remote(ref, ref, s_gly, (k - 1, q - 1, c), at("dp", other))

    def own_share(to):
        return remote(gu_in, gu.at[d] if to else gu.at[other], s_own, (0,), at("dp", other))

    def da(k, to):
        if to:
            dd = lax.rem(d + k, N)
            return remote(dn_in.at[share(dd, g)], stage.at[d], s_da, (k - 1,), at("dp", dd))
        ref = stage.at[lax.rem(d - k + N, N)]
        return remote(ref, ref, s_da, (k - 1,), at("dp", d))

    def staged(tt):
        return stage.at[tt // sub, :, pl.ds(pl.multiple_of(lax.rem(tt, sub) * cols, 128), cols)]

    def db(k, to):
        tt = lax.rem(t + k, T)
        if to:
            return remote(staged(tt), down.at[t, share(d, g)], s_db, (k - 1,), at("tensor", tt))
        ref = down.at[lax.rem(t - k + T, T), share(d, g)]
        return remote(ref, ref, s_db, (k - 1,), at("tensor", t))

    def cx(k, m, to):
        tt = lax.rem(t - k + T, T)
        ref = down.at[tt, share(d if to else dp_of(hi - m, lo), g)]
        return remote(ref, ref, s_cx, (m - 1, k), at("dp", dp_of(hi + m, lo)))

    def cy(k, m, q, to):
        tt = lax.rem(t - k + T, T)
        ref = down.at[tt, share(dp_of(hi - m, lo), g if to else lax.rem(g - q + G, G))]
        return remote(ref, ref, s_cy, (q - 1, m, k), at("groups", lax.rem(g + q, G)))

    def cf(j, k, m, q, to):
        far = lax.rem(g - q + G, G)
        tt = lax.rem(t - k + T, T)
        ref = down.at[tt, share(d if to else dp_of(hi - m, lo), far)]
        return remote(ref, ref, s_cf, (q - 1, m - 1, j), at("dp", dp_of(hi + m, lo)))

    def far_half(j, k):
        for q in range(1, G):
            cy(k, 0, q, False).wait_recv()
            for m in range(1, H):
                cf(j, k, m, q, True).start()

    def cl(k, m, to):
        tt = lax.rem(t - k + T, T)
        dd = dp_of(hi - m, lo if to else lax.rem(lo + 1, L))
        ref = down.at[tt, pl.ds(pl.multiple_of(dd * quarter, 16), quarter)]
        return remote(ref, ref, s_cl, (m, k), at("dp", other))

    def tok_first(c):
        for way in range(2):
            when(tok_can_send(way, 1), lambda way=way: tok_send(way, 1, c, True).start())

    for c in range(HELD, TC):
        tok_first(c)
    for c in range(NC):
        if c == EARLY:
            for k in range(1, N):
                da(k, True).start()
        for k in range(1, H):
            gx(k, c, True).start()
    for c in range(NC - XE, NC):
        for k in range(1, H):
            for q in range(1, G):
                gf(k, q, c, True).start()
    if L > 1:
        own_share(True).start()

    def gu_x(c):
        for k in range(1, H):
            gx(k, c, False).wait_recv()
            for q in range(1, G) if c < NC - XE else ():
                gy(k, q, c, True).start()
            if L > 1:
                glx(k, c, True).start()

    def gu_y(c):
        for k in range(1, H):
            for q in range(1, G):
                (gy if c < NC - XE else gf)(k, q, c, False).wait_recv()
                if L > 1:
                    gly(k, q, c, True).start()

    def meet():
        when(below, lambda: pl.semaphore_wait(s_far.at[0], 1))
        beside(above, 1, s_far.at[0])
        when(above, lambda: pl.semaphore_wait(s_far.at[1], 1))
        beside(below, -1, s_far.at[1])

    if line:
        meet()

    chosen = (lax.broadcasted_iota(jnp.int32, (width, units), 0)
              == 2 * lax.broadcasted_iota(jnp.int32, (width, units), 1))
    pick[...] = jnp.where(chosen, 1.0, 0.0).astype(jnp.bfloat16)

    def dispatch():
        own_stage.wait()
        for k in range(1, N):
            da(k, False).wait_recv()
        loop(1, T, lambda k: db(k, True).start())
        mine = pltpu.make_async_copy(staged(t), down.at[t, share(d, g)], s_loc.at[2])
        mine.start()
        mine.wait()

    def down_z(k, mine):
        if not mine:
            db(k, False).wait_recv()
        for m in range(1, H):
            cx(k, m, True).start()
        for q in range(1, G):
            cy(k, 0, q, True).start()

    def down_x(k, j=None):
        for m in range(1, H):
            cx(k, m, False).wait_recv()
            for q in () if j in FARS else range(1, G):
                cy(k, m, q, True).start()

    def down_y(k, j=None):
        for m in range(H):
            for q in range(1, G):
                if j not in FARS:
                    cy(k, m, q, False).wait_recv()
                elif m:
                    cf(j, k, m, q, False).wait_recv()
            if L > 1:
                cl(k, m, True).start()

    def gu_all():
        own_gu.wait()
        if L > 1:
            own_share(False).wait_recv()
            for k in range(1, H):
                for c in range(NC):
                    glx(k, c, False).wait_recv()
                    for q in range(1, G):
                        gly(k, q, c, False).wait_recv()

    def product(b, part_of=slice(None)):
        at_b = pl.ds(pl.multiple_of(b * feats, 128), feats)
        return jnp.dot(tok[part_of, at_b], gu[b * feats // depth, pl.ds(pl.multiple_of(lax.rem(b * feats, depth), 128), feats)],
                       preferred_element_type=jnp.float32)

    def near(s, waits=False):
        def add(way):
            for c in range(TC if waits else 0):
                when(last_plane(), lambda c=c: tok_recv(way, s, c).wait_recv())
            comb[...] += product(t + s if way else t - s)

        when(t - s >= 0, lambda: add(0))
        when(t + s < T, lambda: add(1))

    def first_products():
        gu_all()
        comb[...] = product(t)
        for s in range(1, T - 1):
            near(s, True)

    def begin():
        dispatch()
        for c in range(HELD):
            tok_first(c)
        down_z(0, True)

    if T <= 8:
        own_tok.wait()
        slots = [0] + [nearest(j, False) for j in range(1, T)]
        steps = {
            BEGINS: begin, GU_X: gu_x, GU_Y: gu_y, PRODUCTS: first_products, TOK_STEP: tok_step,
            DOWN_Z: lambda j: down_z(slots[j], False), DOWN_X: lambda j: down_x(slots[j], j),
            FAR_HALF: lambda j: far_half(j, slots[j]),
        }

        def run(order):
            for kind, *which in order:
                steps[kind](*which)

        ends, others = events(T, NC, TC)
        when(last_plane(), lambda: run(ends))
        when(jnp.logical_not(last_plane()), lambda: run(others))
    else:
        own_tok.wait()
        for c in range(NC):
            gu_x(c)
        begin()
        for c in range(NC):
            gu_y(c)

        def whole_step(s):
            for c in range(TC):
                tok_step(s, c)

        loop(1, T, whole_step)
        loop(1, T, lambda k: down_z(k, False))
        far_half(0, 0)
        down_x(0, 0)
        loop(1, T, down_x)
        gu_all()
        comb[...] = product(t)
        loop(1, T, near)
    def hs(k, c, to):
        ref = hid.at[t if to else lax.rem(t - k + T, T), pl.ds(c * rows, rows)]
        return remote(ref, ref, s_hid, (k - 1, c), at("tensor", lax.rem(t + k, T)))

    def finish(c):
        total = comb[pl.ds(c * rows, rows)]
        up = pltpu.roll(total, width - 1, 1)
        wide = total / (1.0 + jnp.exp(-total)) * up
        even = lax.rem(lax.broadcasted_iota(jnp.int32, wide.shape, 1), 2) == 0
        wide = jnp.where(even, wide, 0.0).astype(jnp.bfloat16)
        hid[t, pl.ds(c * rows, rows)] = jnp.dot(
            wide, pick[...], preferred_element_type=jnp.float32).astype(jnp.bfloat16)

    def last_rows(way, c):
        for p in range(TC):
            tok_recv(way, T - 1, p).wait_recv()
        part_of = pl.ds(c * rows, rows)
        comb[part_of] += product(t + T - 1 if way else t - T + 1, part_of)

    for c in range(1):
        if line and T > 1:
            when(t == T - 1, lambda c=c: last_rows(0, c))
            when(t == 0, lambda c=c: last_rows(1, c))
        finish(c)
        if line:
            for j in range(1, T):
                hs(lax.rem(T - nearest(T - j, False), T), c, True).start()
        else:
            loop(1, T, lambda k, c=c: hs(k, c, True).start())

    def shared(k):
        if L > 1:
            for m in range(H):
                cl(k, m, False).wait_recv()

    def term(k):
        tt = lax.rem(t - k + T, T)
        return jnp.dot(hid[tt], down[tt], preferred_element_type=jnp.float32)

    def mix(k):
        for c in range(1):
            hs(k, c, False).wait_recv()
        acc[...] += term(k)

    if line:
        order = [nearest(j, True) for j in range(1, T)]
        for j in range(T):
            down_y(slots[j], j)
        shared(0)
        acc[...] = term(0)
        for j in range(1, T - 1):
            shared(order[j - 1])
            mix(order[j - 1])
        if T > 1:
            shared(order[-1])
            for c in range(1):
                hs(order[-1], c, False).wait_recv()
            out[...] = (acc[...] + term(order[-1])).astype(out.dtype)
        else:
            out[...] = acc[...].astype(out.dtype)
    else:
        down_y(0, 0)
        loop(1, T, down_y)
        loop(0, T, shared)
        acc[...] = term(0)
        loop(1, T, mix)
        out[...] = acc[...].astype(out.dtype)

    def tok_sent(s):
        for way in range(2):
            for c in range(TC):
                when(tok_can_send(way, s), lambda way=way, c=c: tok_send(way, s, c, False).wait_send())

    loop(1, T, tok_sent)
    for k in range(1, H):
        for c in range(NC):
            gx(k, c, True).wait_send()
            if L > 1:
                glx(k, c, True).wait_send()
            for q in range(1, G):
                (gy if c < NC - XE else gf)(k, q, c, True).wait_send()
                if L > 1:
                    gly(k, q, c, True).wait_send()
    if L > 1:
        own_share(True).wait_send()
    for k in range(1, N):
        da(k, True).wait_send()

    def sent(k):
        db(k, True).wait_send()
        for c in range(1):
            hs(k, c, True).wait_send()

    loop(1, T, sent)

    def plane_sent(k, j=None):
        for m in range(1, H):
            cx(k, m, True).wait_send()
        for m in range(H):
            for q in range(1, G):
                if j in FARS and m:
                    cf(j, k, m, q, True).wait_send()
                else:
                    cy(k, m, q, True).wait_send()
            if L > 1:
                cl(k, m, True).wait_send()

    if line:
        for j in range(T):
            plane_sent(slots[j], j)
    else:
        plane_sent(0, 0)
        loop(1, T, plane_sent)


def per_device(mesh, tokens, gate_up_weight, down_weight):
    G, N, T = (mesh.shape[a] for a in ("groups", "dp", "tensor"))
    L = 2 if N % 2 == 0 else 1
    H = N // L
    NC, TC = 8, 2
    rows, feats = tokens.shape
    depth, width = gate_up_weight.shape
    units = down_weight.shape[0]
    cols = down_weight.shape[1] * N // T
    dma = pltpu.SemaphoreType.DMA
    one = max
    bf = jnp.bfloat16
    sem = lambda *shape: dma((2,) + tuple(one(1, n) for n in shape))
    return pl.pallas_call(
        functools.partial(kernel, (G, N, T, L, H, NC, TC)),
        out_shape=pltpu.VMEM((rows, cols), bf),
        in_specs=[pl.BlockSpec(memory_space=pl.ANY)] * 3,
        out_specs=pl.BlockSpec(memory_space=pltpu.VMEM),
        scratch_shapes=[
            pltpu.VMEM((rows, feats * T), bf),
            pltpu.VMEM((N, depth, width), bf),
            pltpu.VMEM((N, units // N // G, down_weight.shape[1]), bf),
            pltpu.VMEM((T, units, cols), bf),
            pltpu.VMEM((T, rows, units), bf),
            pltpu.VMEM((rows, width), jnp.float32),
            pltpu.VMEM((rows, cols), jnp.float32),
            dma((3,)),
            sem(2, T - 1, TC),
            sem(1),
            sem(H - 1, NC),
            sem(H - 1, G - 1, NC),
            sem(H - 1, NC),
            sem(H - 1, G - 1, NC),
            sem(N - 1),
            sem(T - 1),
            sem(H - 1, T),
            sem(G - 1, H, T),
            sem(H, T),
            sem(T - 1, TC),
            sem(G - 1, H - 1, T),
            pltpu.SemaphoreType.REGULAR((2,)),
            sem(H - 1, G - 1, NC),
            pltpu.VMEM((width, units), bf),
        ],
        compiler_params=pltpu.CompilerParams(collective_id=0, has_side_effects=True,
                                             vmem_limit_bytes=60 * 1024 * 1024),
    )(tokens, gate_up_weight, down_weight)


def solution(mesh):
    in_specs = (P(("groups", "dp"), "tensor"), P("dp", "tensor"), P("tensor", "dp"))
    out_specs = P(("groups", "dp"), "tensor")
    return jax.shard_map(
        functools.partial(per_device, mesh), mesh=mesh, in_specs=in_specs, out_specs=out_specs, check_vma=False
    )
```
